32 devices in a mesh: lat: 8 (over y, x, core), blk: 4 (over z).
Axes of the slice: x: 2, y: 2, z: 4, core: 2. Of those that a mesh axis runs over, the one named last changes fastest.
Arguments:
- mesh_nodes: bfloat16 [10240, 512], P(('lat', 'blk')), may hold values from -6 to 6
- coarse_nodes: bfloat16 [640, 512], replicated, may hold values from -6 to 6
- edge_latents: bfloat16 [65536, 512], P(('lat', 'blk')), may hold values from -6 to 6
- edge_tiles: int32 [512, 2, 128], P(('lat', 'blk')), may hold values from 0 to 1023, as said below
- send_lists: int32 [32, 8, 8], P(('lat', 'blk')), may hold values from 0 to 319
- tiles_live: int32 [32], P(('lat', 'blk')), may hold values from 1 to 16, as said below
- edge_in: bfloat16 [3, 512, 512], replicated, may hold values from -0.15625 to 0.15625
- edge_out: bfloat16 [512, 512], replicated, may hold values from -0.25 to 0.25
- edge_gain: float32 [512], replicated, may hold values from 0.1 to 1.9
- node_in: bfloat16 [2, 512, 512], replicated, may hold values from -0.1875 to 0.1875
- node_out: bfloat16 [512, 512], replicated, may hold values from -0.25 to 0.25
- node_gain: float32 [512], replicated, may hold values from 0.1 to 1.9
- grad_nodes: bfloat16 [10240, 512], P(('lat', 'blk')), may hold values from -6 to 6
- grad_coarse: bfloat16 [640, 512], replicated, may hold values from -6 to 6
- grad_edges: bfloat16 [65536, 512], P(('lat', 'blk')), may hold values from -6 to 6
Outputs:
- new_nodes: bfloat16 [10240, 512], P(('lat', 'blk'))
- new_coarse: bfloat16 [640, 512], replicated
- new_edges: bfloat16 [65536, 512], P(('lat', 'blk'))
- nodes_grad: bfloat16 [10240, 512], P(('lat', 'blk'))
- coarse_grad: bfloat16 [640, 512], replicated
- edges_grad: bfloat16 [65536, 512], P(('lat', 'blk'))
- edge_in_grad: bfloat16 [3, 512, 512], replicated
- edge_out_grad: bfloat16 [512, 512], replicated
- edge_gain_grad: float32 [512], replicated
- node_in_grad: bfloat16 [2, 512, 512], replicated
- node_out_grad: bfloat16 [512, 512], replicated
- node_gain_grad: float32 [512], replicated
The draws below stay inside these ranges and needn't reach their ends.
Inputs may be any that keep to these rules, and one draw needn't show every extreme that they name: `edge_tiles`: sender entries lie below 1024, receiver entries below 960. `send_lists`: numbers of nodes within the sending block. `tiles_live`: some block has all 16 tiles live.
All inputs are finite; a program needn't handle non-finite values.
Results may differ from the reference program's by a relative error of at most 0.0095.
Values may be sent and summed in bfloat16 or wider, within the bound.
A program may use at most 192 MiB of HBM per device.

```python
import jax
import jax.numpy as jnp
from jax import lax

D = 512
NODE_DEV = 320
TILE_DEV = 16
SLOTS = 8
NEIGH = 8
TILE = 128
COARSE = 640
BLOCKS = 32
NODES = 10240
TILES = 512
EDGES = 65536


def draw_edge_tiles(key, part):
    tile_shape = (TILES, TILE)
    subkeys = jax.random.split(jax.random.fold_in(key, 11), 7)
    sender_kind = jax.random.randint(subkeys[0], tile_shape, 0, 20)
    own_ids = jax.random.randint(subkeys[1], tile_shape, 0, NODE_DEV)
    halo_ids = NODE_DEV + jax.random.randint(subkeys[2], tile_shape, 0, NEIGH * SLOTS)
    coarse_ids = NODE_DEV + NEIGH * SLOTS + jax.random.randint(subkeys[3], tile_shape, 0, COARSE)
    senders = jnp.where(sender_kind < 10, own_ids, jnp.where(sender_kind < 17, halo_ids, coarse_ids))
    receiver_kind = jax.random.randint(subkeys[4], tile_shape, 0, 10)
    target_own = jax.random.randint(subkeys[5], tile_shape, 0, NODE_DEV)
    target_coarse = NODE_DEV + jax.random.randint(subkeys[6], tile_shape, 0, COARSE)
    receivers = jnp.where(receiver_kind < 9, target_own, target_coarse)
    return jnp.stack([senders, receivers], axis=1).astype(jnp.int32)


def draw_tiles_live(key, part):
    subkeys = jax.random.split(jax.random.fold_in(key, 23), 3)
    full_flag = jax.random.randint(subkeys[0], (BLOCKS,), 0, 8) == 0
    chosen = jax.random.randint(subkeys[1], (), 0, BLOCKS)
    partial_count = jax.random.randint(subkeys[2], (BLOCKS,), TILE_DEV // 2, TILE_DEV + 1)
    is_full = full_flag | (jnp.arange(BLOCKS) == chosen)
    return jnp.where(is_full, TILE_DEV, partial_count).astype(jnp.int32)


def plant(result, rng, smallest, largest):
    extent = result.shape
    spot = [jax.random.randint(jax.random.fold_in(rng, axis), (), 0, extent[axis]) for axis in range(len(extent))]
    result = result.at[tuple(spot)].set(smallest)
    longest = extent.index(max(extent))
    spot[longest] = (spot[longest] + 1) % extent[longest]
    return result.at[tuple(spot)].set(largest)


def shard_levels(key, extent, pieces, low, largest):
    def one(dim, parts):
        heights = jax.random.uniform(jax.random.fold_in(jax.random.fold_in(key, 6), dim), (parts,), jnp.float32, low / len(pieces), largest / len(pieces))
        return jnp.repeat(jnp.exp(heights), extent[dim] // parts).reshape((-1,) + (1,) * (len(extent) - dim - 1))

    loudness = one(*pieces[0])
    for cut in pieces[1:]:
        loudness = loudness * one(*cut)
    return loudness


def scatter_about(own_key, dims, deviation, reach, pieces=(), kind=jnp.bfloat16):
    loudness = shard_levels(own_key, dims, pieces, -0.22, 0.18) if pieces else 1.0
    result = jax.random.normal(own_key, dims, jnp.float32) * deviation * loudness
    return jnp.minimum(jnp.maximum(result, -reach), reach).astype(kind)


def setup_inputs(seed: int = 0) -> dict:
    seeds = jax.random.split(jax.random.key(seed), 16)
    return {
        "mesh_nodes": scatter_about(seeds[0], (NODES, D), 1.0, 6.0, ((0, 32),)),
        "coarse_nodes": scatter_about(seeds[1], (COARSE, D), 1.0, 6.0),
        "edge_latents": scatter_about(seeds[2], (EDGES, D), 1.0, 6.0, ((0, 32),)),
        "edge_tiles": draw_edge_tiles(jax.random.fold_in(seeds[15], 71), 0),
        "send_lists": plant(jax.random.randint(seeds[4], (BLOCKS, NEIGH, SLOTS), 0, NODE_DEV), jax.random.fold_in(seeds[4], 1), 0, NODE_DEV - 1).astype(jnp.int32),
        "tiles_live": draw_tiles_live(jax.random.fold_in(seeds[15], 71), 0),
        "edge_in": scatter_about(seeds[6], (3, D, D), (3 * D) ** -0.5, 0.15625),
        "edge_out": scatter_about(seeds[7], (D, D), D ** -0.5, 0.25),
        "edge_gain": jnp.clip(1.0 + 0.18 * jax.random.normal(seeds[8], (D,), jnp.float32), 0.1, 1.9),
        "node_in": scatter_about(seeds[9], (2, D, D), (2 * D) ** -0.5, 0.1875),
        "node_out": scatter_about(seeds[10], (D, D), D ** -0.5, 0.25),
        "node_gain": jnp.clip(1.0 + 0.18 * jax.random.normal(seeds[11], (D,), jnp.float32), 0.1, 1.9),
        "grad_nodes": scatter_about(seeds[12], (NODES, D), 1.0, 6.0, ((0, 32),)),
        "grad_coarse": scatter_about(seeds[13], (COARSE, D), 1.0, 6.0),
        "grad_edges": scatter_about(seeds[14], (EDGES, D), 1.0, 6.0, ((0, 32),)),
    }


EPS = 1e-05

def product(first_op, second_op):
    return jnp.dot(first_op, second_op, preferred_element_type=jnp.float32)

def inner_rows(first_op, second_op):
    return lax.dot_general(first_op, second_op, (((0,), (0,)), ((), ())), preferred_element_type=jnp.float32)

def outer_cols(first_op, second_op):
    return lax.dot_general(first_op, second_op, (((1,), (1,)), ((), ())), preferred_element_type=jnp.float32)

def exact_cols(first_op, second_op):
    return lax.dot_general(first_op, second_op, (((1,), (1,)), ((), ())), precision=lax.Precision.HIGHEST, preferred_element_type=jnp.float32)

def normalize(values):
    centered = values - lax.optimization_barrier(jnp.mean(values, axis=-1, keepdims=True))
    inverse = lax.rsqrt(lax.optimization_barrier(jnp.mean(centered * centered, axis=-1, keepdims=True)) + EPS)
    return (centered * inverse, inverse)

def normalize_back(upstream, normed, inverse):
    return inverse * (upstream - lax.optimization_barrier(jnp.mean(upstream, axis=-1, keepdims=True)) - normed * lax.optimization_barrier(jnp.mean(upstream * normed, axis=-1, keepdims=True)))

def swish_slope(values):
    sigmoid_v = jax.nn.sigmoid(values)
    return sigmoid_v * (1.0 + values * (1.0 - sigmoid_v))

def cycle_moves(neigh_count, block_count):
    near_count = neigh_count // 2 - 1
    near = [position - near_count for position in range(near_count)] + [position + 1 for position in range(near_count)]
    return near + [block_count // 4, block_count // 2]

def edge_forward(edge_rows, sender_part, receiver_part, alive_mask, edge_in, edge_out, edge_gain):
    preact = product(edge_rows, edge_in[0]) + sender_part + receiver_part
    hidden = jax.nn.silu(preact).astype(jnp.bfloat16)
    normed, inverse = normalize(product(hidden, edge_out))
    message = normed * edge_gain[None, :] * alive_mask[:, None]
    updated = (edge_rows.astype(jnp.float32) + message).astype(jnp.bfloat16)
    return (preact, hidden, normed, inverse, message, updated)

def edge_backward(edge_rows, preact, hidden, normed, inverse, alive_mask, message_grad, edge_in, edge_out, edge_gain):
    message_grad = message_grad * alive_mask[:, None]
    gain_grad = lax.optimization_barrier(jnp.sum(message_grad * normed, axis=0))
    out_slope = normalize_back(message_grad * edge_gain[None, :], normed, inverse).astype(jnp.bfloat16)
    out_grad = inner_rows(hidden, out_slope)
    pre_slope = (outer_cols(out_slope, edge_out) * swish_slope(preact)).astype(jnp.bfloat16)
    edge_grad = outer_cols(pre_slope, edge_in[0])
    first_grad = inner_rows(edge_rows, pre_slope)
    return (pre_slope, edge_grad, first_grad, out_grad, gain_grad)

def node_forward(node_rows, aggregate, node_in, node_out, node_gain):
    summed = aggregate.astype(jnp.bfloat16)
    preact = product(node_rows, node_in[0]) + product(summed, node_in[1])
    hidden = jax.nn.silu(preact).astype(jnp.bfloat16)
    normed, inverse = normalize(product(hidden, node_out))
    updated = (node_rows.astype(jnp.float32) + normed * node_gain[None, :]).astype(jnp.bfloat16)
    return (summed, preact, hidden, normed, inverse, updated)

def node_backward(node_rows, summed, preact, hidden, normed, inverse, node_slope, node_in, node_out, node_gain):
    gain_grad = lax.optimization_barrier(jnp.sum(node_slope * normed, axis=0))
    out_slope = normalize_back(node_slope * node_gain[None, :], normed, inverse).astype(jnp.bfloat16)
    out_grad = inner_rows(hidden, out_slope)
    pre_slope = (outer_cols(out_slope, node_out) * swish_slope(preact)).astype(jnp.bfloat16)
    direct = node_slope + outer_cols(pre_slope, node_in[0])
    aggregate_grad = outer_cols(pre_slope, node_in[1])
    in_grad = jnp.stack([inner_rows(node_rows, pre_slope), inner_rows(summed, pre_slope)])
    return (direct, aggregate_grad, in_grad, out_grad, gain_grad)

def reference(mesh_nodes, coarse_nodes, edge_latents, edge_tiles, send_lists, tiles_live, edge_in, edge_out, edge_gain, node_in, node_out, node_gain, grad_nodes, grad_coarse, grad_edges):
    block_count = tiles_live.shape[0]
    fine_count, features = mesh_nodes.shape
    node_dev = fine_count // block_count
    neigh_count = send_lists.shape[1]
    slot_count = send_lists.shape[2]
    halo_count = neigh_count * slot_count
    move_table = jnp.array(cycle_moves(neigh_count, block_count), dtype=jnp.int32)
    all_nodes = jnp.concatenate([mesh_nodes, coarse_nodes], axis=0)
    row_count = all_nodes.shape[0]
    sender_proj = product(all_nodes, edge_in[1])
    receiver_proj = product(all_nodes, edge_in[2])
    tile_dev = edge_tiles.shape[0] // block_count
    tile_width = edge_tiles.shape[2]
    edge_blocks = edge_latents.reshape(block_count, tile_dev * tile_width, features)
    tile_blocks = edge_tiles.reshape(block_count, tile_dev, 2, tile_width)
    slope_blocks = grad_edges.reshape(block_count, tile_dev * tile_width, features)
    block_ids = jnp.arange(block_count, dtype=jnp.int32)

    def endpoints(block, tiles):
        senders = tiles[:, 0, :].reshape(-1)
        receivers = tiles[:, 1, :].reshape(-1)
        offset = block * node_dev
        halo_pos = jnp.clip(senders - node_dev, 0, halo_count - 1).astype(jnp.int32)
        neighbour = (halo_pos // slot_count).astype(jnp.int32)
        moved_by = move_table[neighbour].astype(jnp.int32)
        source = ((block + moved_by) % block_count).astype(jnp.int32)
        listed = send_lists[source, neighbour, halo_pos % slot_count]
        sender_ids = jnp.where(senders < node_dev, offset + senders, jnp.where(senders < node_dev + halo_count, source * node_dev + listed, fine_count + senders - node_dev - halo_count))
        receiver_ids = jnp.where(receivers < node_dev, offset + receivers, fine_count + receivers - node_dev)
        alive_flag = jnp.arange(tile_dev, dtype=jnp.int32) < tiles_live[block]
        alive_mask = jnp.broadcast_to(alive_flag[:, None], (tile_dev, tile_width)).reshape(-1).astype(jnp.float32)
        return (sender_ids.astype(jnp.int32), receiver_ids.astype(jnp.int32), alive_mask)

    def forward_block(aggregate, block_data):
        block, edge_rows, tiles = block_data
        sender_ids, receiver_ids, alive_mask = endpoints(block, tiles)
        results = edge_forward(edge_rows, sender_proj[sender_ids], receiver_proj[receiver_ids], alive_mask, edge_in, edge_out, edge_gain)
        aggregate = aggregate + jax.ops.segment_sum(results[4], receiver_ids, num_segments=row_count)
        return (aggregate, results[5])
    zero_rows = jnp.zeros((row_count, features), jnp.float32)
    aggregate, new_edges = lax.scan(forward_block, zero_rows, (block_ids, edge_blocks, tile_blocks))
    summed, preact, hidden, normed, inverse, updated = node_forward(all_nodes, aggregate, node_in, node_out, node_gain)
    node_slope = jnp.concatenate([grad_nodes, grad_coarse], axis=0).astype(jnp.float32)
    direct, aggregate_grad, node_in_sum, node_out_sum, node_gain_sum = node_backward(all_nodes, summed, preact, hidden, normed, inverse, node_slope, node_in, node_out, node_gain)

    def backward_block(carry, block_data):
        sender_slope, receiver_slope, first_sum, sender_sum, receiver_sum, out_sum, gain_sum = carry
        block, edge_rows, tiles, edge_slope = block_data
        sender_ids, receiver_ids, alive_mask = endpoints(block, tiles)
        preact_e, hidden_e, normed_e, inverse_e, message, updated_e = edge_forward(edge_rows, sender_proj[sender_ids], receiver_proj[receiver_ids], alive_mask, edge_in, edge_out, edge_gain)
        message_grad = edge_slope.astype(jnp.float32) + aggregate_grad[receiver_ids]
        pre_slope, edge_grad, first_grad, out_grad, gain_grad = edge_backward(edge_rows, preact_e, hidden_e, normed_e, inverse_e, alive_mask, message_grad, edge_in, edge_out, edge_gain)
        sender_term = inner_rows(all_nodes[sender_ids], pre_slope)
        receiver_term = inner_rows(all_nodes[receiver_ids], pre_slope)
        wide_slope = lax.optimization_barrier(pre_slope).astype(jnp.float32)
        sender_slope = sender_slope + jax.ops.segment_sum(wide_slope, sender_ids, num_segments=row_count)
        receiver_slope = receiver_slope + jax.ops.segment_sum(wide_slope, receiver_ids, num_segments=row_count)
        carry = (sender_slope, receiver_slope, first_sum + first_grad, sender_sum + sender_term, receiver_sum + receiver_term, out_sum + out_grad, gain_sum + gain_grad)
        return (carry, (edge_slope.astype(jnp.float32) + edge_grad).astype(jnp.bfloat16))
    zero_square = jnp.zeros((features, features), jnp.float32)
    start_carry = (zero_rows, zero_rows, zero_square, zero_square, zero_square, zero_square, jnp.zeros((features,), jnp.float32))
    final_carry, edges_grad = lax.scan(backward_block, start_carry, (block_ids, edge_blocks, tile_blocks, slope_blocks))
    sender_slope, receiver_slope, first_sum, sender_sum, receiver_sum, out_sum, gain_sum = final_carry
    node_total = direct + exact_cols(sender_slope, edge_in[1].astype(jnp.float32)) + exact_cols(receiver_slope, edge_in[2].astype(jnp.float32))
    factor = float(edge_latents.shape[0]) ** (-0.5)
    edge_in_grad = (jnp.stack([first_sum, sender_sum, receiver_sum]) * factor).astype(jnp.bfloat16)
    return (updated[:fine_count], updated[fine_count:], new_edges.reshape(edge_latents.shape), node_total[:fine_count].astype(jnp.bfloat16), node_total[fine_count:].astype(jnp.bfloat16), edges_grad.reshape(edge_latents.shape), edge_in_grad, (out_sum * factor).astype(jnp.bfloat16), gain_sum * factor, (node_in_sum * factor).astype(jnp.bfloat16), (node_out_sum * factor).astype(jnp.bfloat16), node_gain_sum * factor)
```

```python
import functools

import jax
import jax.numpy as jnp
from jax import lax
from jax.experimental import pallas as pl
from jax.experimental.pallas import tpu as pltpu
from jax.sharding import PartitionSpec as P

EPS = 1e-05
BF = jnp.bfloat16
F32 = jnp.float32
AXES = ("lat", "blk")
MESH = pl.DeviceIdType.MESH


def dims(a, b, ca, cb):
    return lax.dot_general(a, b, (((ca,), (cb,)), ((), ())), preferred_element_type=F32)


def product(a, b):
    return dims(a, b, 1, 0)


def inner_rows(a, b):
    return dims(a, b, 0, 0)


def outer_cols(a, b):
    return dims(a, b, 1, 1)


def normalize(values):
    centered = values - jnp.mean(values, axis=-1, keepdims=True)
    inverse = lax.rsqrt(jnp.mean(centered * centered, axis=-1, keepdims=True) + EPS)
    return (centered * inverse, inverse)


def normalize_back(upstream, normed, inverse):
    return inverse * (
        upstream
        - jnp.mean(upstream, axis=-1, keepdims=True)
        - normed * jnp.mean(upstream * normed, axis=-1, keepdims=True)
    )


def one_hot(index, shape, axis):
    return jnp.where(lax.broadcasted_iota(jnp.int32, shape, axis) == index, 1.0, 0.0).astype(BF)


def cycle_moves(neigh_count, block_count):
    near_count = neigh_count // 2 - 1
    near = [position - near_count for position in range(near_count)] + [
        position + 1 for position in range(near_count)
    ]
    return near + [block_count // 4, block_count // 2]


def square_bits(sizes):
    found = []
    for axis, size in zip(AXES, sizes):
        step = 1
        while step < size:
            found.append((axis, step))
            step *= 2
        assert step == size
    return found


def turned(bits, turn):
    middle = bits[1:-1]
    turn = turn % len(middle)
    return [bits[0]] + middle[turn:] + middle[:turn] + [bits[-1]]


def bit_of(place, bit):
    return lax.rem(place[bit[0]] // bit[1], 2)


def across(place, bit):
    axis, step = bit
    moved = dict(place)
    moved[axis] = place[axis] + step - 2 * step * bit_of(place, bit)
    return tuple(moved[axis] for axis in AXES)


def here():
    return {axis: lax.axis_index(axis) for axis in AXES}


class Fold:
    def __init__(self, place, order, source, target, lo, rows, cols, arrive, held, sems):
        self.place, self.order = place, order
        self.source, self.target, self.lo = source, target, lo
        self.rows, self.cols = rows, cols
        self.arrive, self.held = arrive, held
        self.rs_send, self.rs_recv, self.ag_send, self.ag_recv = sems

    @staticmethod
    def shapes(count, rows, cols):
        found = []
        for stage in range(count):
            if stage < 2:
                cols //= 2
            else:
                rows //= 2
            found.append((rows, cols))
        return found

    def halves(self, stage):
        rows, cols = self.shapes(len(self.order), self.rows, self.cols)[stage]
        bit = bit_of(self.place, self.order[stage])
        if stage < 2:
            mine, other = pl.multiple_of(bit * cols, 128), pl.multiple_of((1 - bit) * cols, 128)
            return rows, (0, pl.ds(mine, cols)), (0, pl.ds(other, cols))
        mine, other = pl.multiple_of(bit * rows, 16), pl.multiple_of((1 - bit) * rows, 16)
        return rows, (mine, pl.ds(0, cols)), (other, pl.ds(0, cols))

    def previous(self, stage):
        return (self.source, self.lo) if stage == 0 else (self.held[stage - 1], 0)

    def reduce_copy(self, stage):
        rows, _, (start, span) = self.halves(stage)
        ref, base = self.previous(stage)
        return pltpu.make_async_remote_copy(
            src_ref=ref.at[pl.ds(base + start, rows), span],
            dst_ref=self.arrive[stage],
            send_sem=self.rs_send.at[stage],
            recv_sem=self.rs_recv.at[stage],
            device_id=across(self.place, self.order[stage]),
            device_id_type=MESH,
        )

    def add(self, stage):
        rows, (start, span), _ = self.halves(stage)
        ref, base = self.previous(stage)
        last = stage == len(self.order) - 1
        piece = next(size for size in (128, 80, 64, 48, 32, 16) if rows % size == 0)
        if last:
            row_at, col_at = self.corner(len(self.order))
            cols = self.arrive[stage].shape[1]

        def one(step, carry):
            at = pl.multiple_of(step * piece, 16)
            total = ref[pl.ds(base + start + at, piece), span].astype(F32) + self.arrive[stage][
                pl.ds(at, piece), :
            ].astype(F32)
            if last:
                self.target[pl.ds(row_at + at, piece), pl.ds(col_at, cols)] = total.astype(BF)
            else:
                self.held[stage][pl.ds(at, piece), :] = total.astype(BF)
            return carry

        if rows == piece:
            one(0, 0)
        else:
            lax.fori_loop(0, rows // piece, one, 0)

    def corner(self, stages):
        row, col = self.lo, 0
        for stage in range(stages):
            rows, cols = self.shapes(len(self.order), self.rows, self.cols)[stage]
            bit = bit_of(self.place, self.order[stage])
            if stage < 2:
                col = col + bit * cols
            else:
                row = row + bit * rows
        return pl.multiple_of(row, 16), pl.multiple_of(col, 128)

    def gather_copy(self, stage):
        rows, cols = self.shapes(len(self.order), self.rows, self.cols)[stage]
        row, col = self.corner(stage + 1)
        span = self.target.at[pl.ds(row, rows), pl.ds(col, cols)]
        return pltpu.make_async_remote_copy(
            src_ref=span,
            dst_ref=span,
            send_sem=self.ag_send.at[stage],
            recv_sem=self.ag_recv.at[stage],
            device_id=across(self.place, self.order[stage]),
            device_id_type=MESH,
        )


def fold_scratch(count, parts, cols):
    scratch = []
    for _, _, rows, _ in parts:
        shapes = Fold.shapes(count, rows, cols)
        scratch += [pltpu.VMEM(shape, BF) for shape in shapes]
        scratch += [pltpu.VMEM(shape, BF) for shape in shapes[:-1]]
        scratch += [pltpu.SemaphoreType.DMA((count,))] * 4
    return scratch


def make_folds(place, bits, parts, refs, cols):
    count, folds = len(bits), []
    for number, (source, target, rows, lo) in enumerate(parts):
        mine = refs[: 2 * count + 3]
        refs = refs[2 * count + 3 :]
        folds.append(
            Fold(
                place,
                turned(bits, number),
                source,
                target,
                lo,
                rows,
                cols,
                mine[:count],
                mine[count : 2 * count - 1],
                mine[2 * count - 1 :],
            )
        )
    return folds


def fold_all(folds):
    count = len(folds[0].order)
    for stage in range(count):
        copies = [fold.reduce_copy(stage) for fold in folds]
        for copy in copies:
            copy.start()
        for fold, copy in zip(folds, copies):
            copy.wait()
            fold.add(stage)
    for stage in reversed(range(count)):
        copies = [fold.gather_copy(stage) for fold in folds]
        for copy in copies:
            copy.start()
        for copy in copies:
            copy.wait()


def greet(devices):
    barrier = pltpu.get_barrier_semaphore()
    for device in devices:
        pl.semaphore_signal(barrier, inc=1, device_id=device, device_id_type=MESH)
    pl.semaphore_wait(barrier, len(devices))


def split_rows(rows, count, pieces):
    unit = 16 * 2 ** (count - 2)
    units = -(-rows // unit)
    pieces = min(pieces, units)
    sizes = [unit * (units // pieces + (1 if i < units % pieces else 0)) for i in range(pieces)]
    return sizes


def padded(rows, count):
    return sum(split_rows(rows, count, 1))


def block_at(place, sizes, move):
    total = sizes[0] * sizes[1]
    block = lax.rem(place[AXES[0]] * sizes[1] + place[AXES[1]] + (move % total), total)
    return block // sizes[1], lax.rem(block, sizes[1])


def halo_step(sizes, moves, listed_ref, mesh_ref, halo_ref, out, landed, send, recv):
    place = here()
    greet([block_at(place, sizes, move) for move in moves])
    slots = out.shape[1]
    own = mesh_ref.shape[0]
    pick = one_hot(listed_ref[...], (own, listed_ref.shape[1]), 0)
    rows = inner_rows(pick, mesh_ref[...]).astype(BF)
    copies = []
    for k, move in enumerate(moves):
        out[k] = rows[k * slots : (k + 1) * slots]
    for k, move in enumerate(moves):
        copy = pltpu.make_async_remote_copy(
            src_ref=out.at[k],
            dst_ref=landed.at[k],
            send_sem=send.at[k],
            recv_sem=recv.at[k],
            device_id=block_at(place, sizes, -move),
            device_id_type=MESH,
        )
        copy.start()
        copies.append(copy)
    for copy in copies:
        copy.wait()
    halo_ref[...] = landed[...]


def sum_step(bits, lo_rows, part_ref, out_ref, *refs):
    place = here()
    greet([across(place, bit) for bit in bits])
    cols = part_ref.shape[1]
    parts, lo = [], 0
    for rows in lo_rows:
        parts.append((part_ref, out_ref, rows, lo))
        lo += rows
    fold_all(make_folds(place, bits, parts, refs, cols))


def final_step(
    bits,
    sizes,
    moves,
    lo_rows,
    edge_ref,
    node_ref,
    term_ref,
    listed_ref,
    direct_ref,
    edge_out,
    node_out,
    nodes_grad,
    landed,
    send,
    recv,
    *refs,
):
    place = here()
    greet([across(place, bit) for bit in bits] + [block_at(place, sizes, -move) for move in moves])
    copies = []
    for k, move in enumerate(moves):
        copy = pltpu.make_async_remote_copy(
            src_ref=term_ref.at[k],
            dst_ref=landed.at[k],
            send_sem=send.at[k],
            recv_sem=recv.at[k],
            device_id=block_at(place, sizes, move),
            device_id_type=MESH,
        )
        copy.start()
        copies.append(copy)
    cols = edge_ref.shape[1]
    parts, lo = [], 0
    for rows in lo_rows:
        parts.append((edge_ref, edge_out, rows, lo))
        lo += rows
    parts.append((node_ref, node_out, node_ref.shape[0], 0))
    folds = make_folds(place, bits, parts, refs, cols)
    fold_all(folds)
    for copy in copies:
        copy.wait()
    own = direct_ref.shape[0]
    pick = one_hot(listed_ref[...], (own, listed_ref.shape[1]), 0)
    back = landed[...].reshape(listed_ref.shape[1], cols)
    nodes_grad[...] = (direct_ref[...] + product(pick, back)).astype(BF)


def edge_index(tiles_ref, own, halo):
    count, _, width = tiles_ref.shape
    flat = tiles_ref[...].reshape(2 * count, width)
    fine = jnp.where(flat < own, flat, flat + halo)
    row = lax.broadcasted_iota(jnp.int32, flat.shape, 0)
    flat = jnp.where(lax.rem(row, 2) == 0, flat, fine)
    turned_flat = flat.T
    send_col = jnp.concatenate([turned_flat[:, 2 * t : 2 * t + 1] for t in range(count)], axis=0)
    recv_col = jnp.concatenate([turned_flat[:, 2 * t + 1 : 2 * t + 2] for t in range(count)], axis=0)
    send_row = jnp.concatenate([flat[2 * t : 2 * t + 1, :] for t in range(count)], axis=1)
    recv_row = jnp.concatenate([flat[2 * t + 1 : 2 * t + 2, :] for t in range(count)], axis=1)
    return send_col, recv_col, send_row, recv_row


def edge_forward(
    tile_width,
    live_ref,
    lat_ref,
    tiles_ref,
    mesh_ref,
    halo_ref,
    coarse_ref,
    win_ref,
    wout_ref,
    gain_ref,
    new_ref,
    hid_ref,
    slope_ref,
    norm_ref,
    inv_ref,
    agg_own,
    agg_coarse,
    proj_s,
    proj_r,
    agg,
):
    step = pl.program_id(0)
    own, halo = mesh_ref.shape[0], halo_ref.shape[0]
    rows = agg.shape[0]
    block = lat_ref.shape[0]

    @pl.when(step == 0)
    def _():
        agg[...] = jnp.zeros_like(agg)
        for part, lo in ((mesh_ref, 0), (halo_ref, own), (coarse_ref, own + halo)):
            span = pl.ds(lo, part.shape[0])
            proj_s[span, :] = product(part[...], win_ref[1]).astype(BF)
            proj_r[span, :] = product(part[...], win_ref[2]).astype(BF)

    send_col, recv_col, _, recv_row = edge_index(tiles_ref, own, halo)
    rows_in = lat_ref[...]
    pre = (
        product(rows_in, win_ref[0])
        + product(one_hot(send_col, (block, rows), 1), proj_s[...])
        + product(one_hot(recv_col, (block, rows), 1), proj_r[...])
    )
    sig = 1.0 / (1.0 + jnp.exp(-pre))
    hidden = (pre * sig).astype(BF)
    slope_ref[...] = (sig * (1.0 + pre * (1.0 - sig))).astype(BF)
    hid_ref[...] = hidden
    normed, inverse = normalize(product(hidden, wout_ref[...]))
    norm_ref[...] = normed.astype(BF)
    inv_ref[...] = inverse
    place = step * block + lax.broadcasted_iota(jnp.int32, (block, 1), 0)
    alive = jnp.where(place < live_ref[0] * tile_width, 1.0, 0.0)
    message = normed * gain_ref[...] * alive
    new_ref[...] = (rows_in.astype(F32) + message).astype(BF)
    agg[...] += product(one_hot(recv_row, (rows, block), 0), message.astype(BF))

    @pl.when(step == pl.num_programs(0) - 1)
    def _():
        agg_own[...] = agg[pl.ds(0, own), :].astype(BF)
        agg_coarse[...] = agg[pl.ds(own + halo, rows - own - halo), :].astype(BF)


def edge_backward(
    tile_width,
    factor,
    live_ref,
    lat_ref,
    grad_ref,
    hid_ref,
    slope_ref,
    norm_ref,
    inv_ref,
    tiles_ref,
    mesh_ref,
    halo_ref,
    coarse_ref,
    own_slope,
    coarse_slope,
    own_direct,
    coarse_direct,
    win_ref,
    wout_ref,
    gain_ref,
    edges_grad,
    pack,
    own_term,
    halo_term,
    table,
    sent,
    received,
    first_acc,
    out_acc,
    gain_grad,
):
    step = pl.program_id(0)
    own, halo = mesh_ref.shape[0], halo_ref.shape[0]
    rows = table.shape[0]
    block = lat_ref.shape[0]

    @pl.when(step == 0)
    def _():
        for acc in (sent, received, first_acc, out_acc, gain_grad):
            acc[...] = jnp.zeros_like(acc)
        table[pl.ds(0, own), :] = own_slope[...]
        table[pl.ds(own, halo), :] = jnp.zeros((halo, table.shape[1]), BF)
        table[pl.ds(own + halo, rows - own - halo), :] = coarse_slope[...]

    _, recv_col, send_row, recv_row = edge_index(tiles_ref, own, halo)
    place = step * block + lax.broadcasted_iota(jnp.int32, (block, 1), 0)
    alive = jnp.where(place < live_ref[0] * tile_width, 1.0, 0.0)
    edge_slope = grad_ref[...].astype(F32)
    message_slope = (
        edge_slope + product(one_hot(recv_col, (block, rows), 1), table[...])
    ) * alive
    normed = norm_ref[...].astype(F32)
    gain_grad[...] += jnp.sum(message_slope * normed, axis=0, keepdims=True)
    out_slope = normalize_back(message_slope * gain_ref[...], normed, inv_ref[...]).astype(BF)
    out_acc[...] += inner_rows(hid_ref[...], out_slope)
    pre_slope = (outer_cols(out_slope, wout_ref[...]) * slope_ref[...].astype(F32)).astype(BF)
    edges_grad[...] = (edge_slope + outer_cols(pre_slope, win_ref[0])).astype(BF)
    first_acc[...] += inner_rows(lat_ref[...], pre_slope)
    sent[...] += product(one_hot(send_row, (rows, block), 0), pre_slope)
    received[...] += product(one_hot(recv_row, (rows, block), 0), pre_slope)

    @pl.when(step == pl.num_programs(0) - 1)
    def _():
        d = first_acc.shape[0]
        coarse = coarse_ref.shape[0]
        pack[pl.ds(0, d), :] = (first_acc[...] * factor).astype(BF)
        pack[pl.ds(3 * d, d), :] = (out_acc[...] * factor).astype(BF)
        sums = [None, None]
        for part, lo in ((mesh_ref, 0), (halo_ref, own), (coarse_ref, own + halo)):
            span = pl.ds(lo, part.shape[0])
            total = None
            for which, source in enumerate((sent, received)):
                piece = source[span, :].astype(BF)
                weight = inner_rows(part[...], piece)
                sums[which] = weight if sums[which] is None else sums[which] + weight
                back = outer_cols(piece, win_ref[1 + which])
                total = back if total is None else total + back
            if part is mesh_ref:
                own_term[...] = total + own_direct[...]
            elif part is halo_ref:
                halo_term[...] = total.astype(BF)
            else:
                pack[pl.ds(4 * d, coarse), :] = (total + coarse_direct[...]).astype(BF)
        pack[pl.ds(d, d), :] = (sums[0] * factor).astype(BF)
        pack[pl.ds(2 * d, d), :] = (sums[1] * factor).astype(BF)
        rest = pack.shape[0] - 4 * d - coarse
        pack[pl.ds(4 * d + coarse, rest), :] = jnp.broadcast_to(gain_grad[...] * factor, (rest, d)).astype(BF)


def node_step(
    masked,
    factor,
    me_ref,
    rows_ref,
    sum_ref,
    grad_ref,
    win_ref,
    wout_ref,
    gain_ref,
    *refs,
):
    if masked:
        base, new_ref, direct_ref, agg_grad, pack, in_grad, out_grad, gain_grad = refs
    else:
        new_ref, direct_ref, agg_grad, in_grad, out_grad, gain_grad = refs

    @pl.when(pl.program_id(0) == 0)
    def _():
        for acc in (in_grad, out_grad, gain_grad):
            acc[...] = jnp.zeros_like(acc)

    rows = rows_ref[...]
    summed = sum_ref[...]
    pre = product(rows, win_ref[0]) + product(summed, win_ref[1])
    sig = 1.0 / (1.0 + jnp.exp(-pre))
    hidden = (pre * sig).astype(BF)
    normed, inverse = normalize(product(hidden, wout_ref[...]))
    new_ref[...] = (rows.astype(F32) + normed * gain_ref[...]).astype(BF)
    node_slope = grad_ref[...].astype(F32)
    out_slope = normalize_back(node_slope * gain_ref[...], normed, inverse).astype(BF)
    swish = sig * (1.0 + pre * (1.0 - sig))
    pre_slope = (outer_cols(out_slope, wout_ref[...]) * swish).astype(BF)
    agg_grad[...] = outer_cols(pre_slope, win_ref[1]).astype(BF)
    direct = node_slope + outer_cols(pre_slope, win_ref[0])
    if masked:
        count, block = me_ref[1], rows.shape[0]
        place = pl.program_id(0) * block + lax.broadcasted_iota(jnp.int32, (block, 1), 0)
        share = jnp.where((place * count) // (pl.num_programs(0) * block) == me_ref[0], 1.0, 0.0)
        direct = direct * share
        node_slope = node_slope * share
        hidden = (hidden.astype(F32) * share).astype(BF)
        pre_slope = (pre_slope.astype(F32) * share).astype(BF)
    direct_ref[...] = direct
    gain_grad[...] += jnp.sum(node_slope * normed, axis=0, keepdims=True)
    out_grad[...] += inner_rows(hidden, out_slope)
    in_grad[0] += inner_rows(rows, pre_slope)
    in_grad[1] += inner_rows(summed, pre_slope)
    if masked:

        @pl.when(pl.program_id(0) == pl.num_programs(0) - 1)
        def _():
            d = in_grad.shape[1]
            for i in range(2):
                pack[pl.ds(i * d, d), :] = ((in_grad[i] + base[pl.ds(i * d, d), :]) * factor).astype(BF)
            pack[pl.ds(2 * d, d), :] = ((out_grad[...] + base[pl.ds(2 * d, d), :]) * factor).astype(BF)
            rest = pack.shape[0] - 3 * d
            gain = (gain_grad[...] + base[pl.ds(3 * d, 1), :]) * factor
            pack[pl.ds(3 * d, rest), :] = jnp.broadcast_to(gain, (rest, d)).astype(BF)


def whole(shape):
    zero = (0,) * len(shape)
    return pl.BlockSpec(shape, lambda i: zero)


def by_rows(block, width):
    return pl.BlockSpec((block, width), lambda i: (i, 0))


def by_cols(block):
    return pl.BlockSpec((1, block), lambda i: (0, i))


def shape_of(shape, dtype):
    return jax.ShapeDtypeStruct(shape, dtype)


def cost(flops, moved):
    return pl.CostEstimate(flops=int(flops), bytes_accessed=int(moved), transcendentals=0)


PARAMS = dict(
    compiler_params=pltpu.CompilerParams(
        dimension_semantics=("arbitrary",), vmem_limit_bytes=60 * 1024 * 1024
    )
)


def talking(number):
    return pltpu.CompilerParams(
        collective_id=number, has_side_effects=True, vmem_limit_bytes=60 * 1024 * 1024
    )


def node_call(me, rows, summed, grad, node_in, node_out, gain, block, factor, base=None, pack_rows=0):
    count, d = rows.shape
    row = by_rows(block, d)
    masked = base is not None
    smem = pl.BlockSpec(memory_space=pltpu.SMEM)
    accs = [(2, d, d), (d, d), (1, d)]
    extra_in = [whole(base.shape)] if masked else []
    acc_specs = [whole((pack_rows, d))] if masked else [whole(shape) for shape in accs]
    acc_shapes = [shape_of((pack_rows, d), BF)] if masked else [shape_of(shape, F32) for shape in accs]
    return pl.pallas_call(
        functools.partial(node_step, masked, factor),
        grid=(count // block,),
        in_specs=[smem, row, row, row, whole((2, d, d)), whole((d, d)), whole((1, d))] + extra_in,
        out_specs=[row, row, row] + acc_specs,
        out_shape=[shape_of((count, d), BF), shape_of((count, d), F32), shape_of((count, d), BF)] + acc_shapes,
        scratch_shapes=[pltpu.VMEM(shape, F32) for shape in accs] if masked else [],
        cost_estimate=cost(18 * count * d * d, 12 * count * d),
        **PARAMS,
    )(me, rows, summed, grad, node_in, node_out, gain, *([base] if masked else []))


def on_device(
    mesh_nodes,
    coarse_nodes,
    edge_latents,
    edge_tiles,
    send_lists,
    tiles_live,
    edge_in,
    edge_out,
    edge_gain,
    node_in,
    node_out,
    node_gain,
    grad_nodes,
    grad_coarse,
    grad_edges,
):
    sizes = tuple(lax.axis_size(axis) for axis in AXES)
    block_count = sizes[0] * sizes[1]
    bits = square_bits(sizes)
    count = len(bits)
    own, d = mesh_nodes.shape
    neigh, slots = send_lists.shape[1:]
    coarse = coarse_nodes.shape[0]
    halo = neigh * slots
    rows = own + halo + coarse
    tile_dev, _, tile_width = edge_tiles.shape
    edges = tile_dev * tile_width
    tiles = 4 if tile_dev % 4 == 0 else 1
    block = tiles * tile_width
    moves = cycle_moves(neigh, block_count)
    factor = float(edges * block_count) ** (-0.5)
    listed = send_lists.reshape(1, halo)
    me = jnp.stack([lax.axis_index("lat") * sizes[1] + lax.axis_index("blk"), jnp.int32(block_count)])
    e_gain, n_gain = edge_gain.reshape(1, d), node_gain.reshape(1, d)
    vmem = pl.BlockSpec(memory_space=pltpu.VMEM)
    incoming = pl.pallas_call(
        functools.partial(halo_step, sizes, moves),
        in_specs=[vmem, vmem],
        out_specs=vmem,
        out_shape=shape_of((neigh, slots, d), BF),
        scratch_shapes=[pltpu.VMEM((neigh, slots, d), BF)] * 2 + [pltpu.SemaphoreType.DMA((neigh,))] * 2,
        compiler_params=talking(0),
    )(listed, mesh_nodes).reshape(halo, d)

    smem = pl.BlockSpec(memory_space=pltpu.SMEM)
    wide, col = by_rows(block, d), by_rows(block, 1)
    pairs = pl.BlockSpec((tiles, 2, tile_width), lambda i: (i, 0, 0))
    tables = [whole((own, d)), whole((halo, d)), whole((coarse, d))]
    weights = [whole((3, d, d)), whole((d, d)), whole((1, d))]
    new_edges, hidden, slope, normed, inverse, agg_own, agg_coarse = pl.pallas_call(
        functools.partial(edge_forward, tile_width),
        grid=(edges // block,),
        in_specs=[smem, wide, pairs] + tables + weights,
        out_specs=[wide] * 4 + [col, whole((own, d)), whole((coarse, d))],
        out_shape=[shape_of((edges, d), BF)] * 4
        + [shape_of((edges, 1), F32), shape_of((own, d), BF), shape_of((coarse, d), BF)],
        scratch_shapes=[
            pltpu.VMEM((rows, d), BF),
            pltpu.VMEM((rows, d), BF),
            pltpu.VMEM((rows, d), F32),
        ],
        cost_estimate=cost(2 * edges * d * (3 * rows + 2 * d), 12 * edges * d),
        **PARAMS,
    )(tiles_live, edge_latents, edge_tiles, mesh_nodes, incoming, coarse_nodes, edge_in, edge_out, e_gain)
    sum_rows = padded(coarse, count)
    if sum_rows > coarse:
        agg_coarse = jnp.pad(agg_coarse, ((0, sum_rows - coarse), (0, 0)))
    coarse_rows = split_rows(sum_rows, count, 3)
    coarse_parts = [(None, None, part, 0) for part in coarse_rows]
    coarse_total = pl.pallas_call(
        functools.partial(sum_step, bits, coarse_rows),
        in_specs=[vmem],
        out_specs=vmem,
        out_shape=shape_of((sum_rows, d), BF),
        scratch_shapes=fold_scratch(count, coarse_parts, d),
        compiler_params=talking(1),
    )(agg_coarse)[:coarse]
    new_nodes, own_direct, own_slope, own_in, own_out, own_ngain = node_call(
        me, mesh_nodes, agg_own, grad_nodes, node_in, node_out, n_gain, own, factor
    )
    base = jnp.concatenate([own_in.reshape(2 * d, d), own_out, jnp.broadcast_to(own_ngain, (8, d))], axis=0)
    c_block = own if coarse % own == 0 else coarse
    node_rows = padded(3 * d + 1, count)
    new_coarse, c_direct, c_slope, node_pack = node_call(
        me, coarse_nodes, coarse_total, grad_coarse, node_in, node_out, n_gain, c_block, factor, base, node_rows
    )
    edge_rows = padded(4 * d + coarse + 1, count)
    edges_grad, edge_pack, own_term, halo_term = pl.pallas_call(
        functools.partial(edge_backward, tile_width, factor),
        grid=(edges // block,),
        in_specs=[smem] + [wide] * 5 + [col, pairs] + tables
        + [whole((own, d)), whole((coarse, d))] * 2 + weights,
        out_specs=[wide, whole((edge_rows, d)), whole((own, d)), whole((halo, d))],
        out_shape=[
            shape_of((edges, d), BF),
            shape_of((edge_rows, d), BF),
            shape_of((own, d), F32),
            shape_of((halo, d), BF),
        ],
        scratch_shapes=[
            pltpu.VMEM((rows, d), BF),
            pltpu.VMEM((rows, d), F32),
            pltpu.VMEM((rows, d), F32),
            pltpu.VMEM((d, d), F32),
            pltpu.VMEM((d, d), F32),
            pltpu.VMEM((1, d), F32),
        ],
        cost_estimate=cost(2 * edges * d * (3 * rows + 4 * d), 14 * edges * d),
        **PARAMS,
    )(
        tiles_live, edge_latents, grad_edges, hidden, slope, normed, inverse, edge_tiles, mesh_nodes, incoming,
        coarse_nodes, own_slope, c_slope, own_direct, c_direct, edge_in, edge_out, e_gain,
    )
    cuts = split_rows(edge_rows, count, 2)
    parts = [(None, None, part, 0) for part in cuts + [node_rows]]
    edge_sum, node_sum, nodes_grad = pl.pallas_call(
        functools.partial(final_step, bits, sizes, moves, cuts),
        in_specs=[vmem] * 5,
        out_specs=[vmem] * 3,
        out_shape=[shape_of((edge_rows, d), BF), shape_of((node_rows, d), BF), shape_of((own, d), BF)],
        scratch_shapes=[pltpu.VMEM((neigh, slots, d), BF)]
        + [pltpu.SemaphoreType.DMA((neigh,))] * 2
        + fold_scratch(count, parts, d),
        compiler_params=talking(2),
    )(edge_pack, node_pack, halo_term.reshape(neigh, slots, d), listed, own_term)
    return (
        new_nodes,
        new_coarse,
        new_edges,
        nodes_grad,
        edge_sum[4 * d : 4 * d + coarse],
        edges_grad,
        edge_sum[: 3 * d].reshape(3, d, d),
        edge_sum[3 * d : 4 * d],
        edge_sum[4 * d + coarse].astype(F32),
        node_sum[: 2 * d].reshape(2, d, d),
        node_sum[2 * d : 3 * d],
        node_sum[3 * d].astype(F32),
    )


def solution(mesh):
    rows2 = P(AXES, None)
    rows3 = P(AXES, None, None)
    in_specs = (
        rows2, P(), rows2, rows3, rows3, P(AXES), P(), P(), P(), P(), P(), P(), rows2, P(), rows2,
    )
    out_specs = (rows2, P(), rows2, rows2, P(), rows2, P(), P(), P(), P(), P(), P())
    return jax.shard_map(
        on_device, mesh=mesh, in_specs=in_specs, out_specs=out_specs, check_vma=False
    )
```

```python
import functools

import jax
import jax.numpy as jnp
from jax import lax
from jax.experimental import pallas as pl
from jax.experimental.pallas import tpu as pltpu
from jax.sharding import PartitionSpec as P

EPS = 1e-05
BF = jnp.bfloat16
F32 = jnp.float32
AXES = ("lat", "blk")
MESH = pl.DeviceIdType.MESH


def dims(a, b, ca, cb):
    return lax.dot_general(a, b, (((ca,), (cb,)), ((), ())), preferred_element_type=F32)


def product(a, b):
    return dims(a, b, 1, 0)


def inner_rows(a, b):
    return dims(a, b, 0, 0)


def outer_cols(a, b):
    return dims(a, b, 1, 1)


def normalize(values):
    centered = values - jnp.mean(values, axis=-1, keepdims=True)
    inverse = lax.rsqrt(jnp.mean(centered * centered, axis=-1, keepdims=True) + EPS)
    return (centered * inverse, inverse)


def normalize_back(upstream, normed, inverse):
    return inverse * (
        upstream
        - jnp.mean(upstream, axis=-1, keepdims=True)
        - normed * jnp.mean(upstream * normed, axis=-1, keepdims=True)
    )


def one_hot(index, shape, axis):
    return jnp.where(lax.broadcasted_iota(jnp.int32, shape, axis) == index, 1.0, 0.0).astype(BF)


def cycle_moves(neigh_count, block_count):
    near_count = neigh_count // 2 - 1
    near = [position - near_count for position in range(near_count)] + [
        position + 1 for position in range(near_count)
    ]
    return near + [block_count // 4, block_count // 2]


def square_bits(sizes):
    found = []
    for axis, size in zip(AXES, sizes):
        step = 1
        while step < size:
            found.append((axis, step))
            step *= 2
        assert step == size
    return found


def turned(bits, turn):
    middle = bits[1:-1]
    turn = turn % len(middle)
    return [bits[0]] + middle[turn:] + middle[:turn] + [bits[-1]]


def bit_of(place, bit):
    return lax.rem(place[bit[0]] // bit[1], 2)


def across(place, bit):
    axis, step = bit
    moved = dict(place)
    moved[axis] = place[axis] + step - 2 * step * bit_of(place, bit)
    return tuple(moved[axis] for axis in AXES)


def here():
    return {axis: lax.axis_index(axis) for axis in AXES}


class Fold:
    def __init__(self, place, order, kinds, source, target, lo, rows, cols, refs, wide_first=False):
        count = len(order)
        self.place, self.order, self.kinds = place, order, kinds
        self.source, self.target, self.lo = source, target, lo
        self.rows, self.cols = rows, cols
        self.arrive, self.held = refs[:count], refs[count : 2 * count - 1]
        self.rs_send, self.rs_recv, self.ag_send, self.ag_recv = refs[2 * count - 1 : 2 * count + 3]
        self.sizes = Fold.shapes(kinds, rows, cols)
        self.gather_order = list(reversed(range(count)))
        if wide_first:
            self.gather_order.sort(key=lambda stage: kinds[stage] == "r")

    @staticmethod
    def shapes(kinds, rows, cols):
        found = []
        for kind in kinds:
            if kind == "c":
                cols //= 2
            else:
                rows //= 2
            found.append((rows, cols))
        return found

    @staticmethod
    def scratch(kinds, rows, cols):
        shapes, count = Fold.shapes(kinds, rows, cols), len(kinds)
        return (
            [pltpu.VMEM(shape, BF) for shape in shapes]
            + [pltpu.VMEM(shape, BF) for shape in shapes[:-1]]
            + [pltpu.SemaphoreType.DMA((count,))] * 4
        )

    def halves(self, stage):
        rows, cols = self.sizes[stage]
        bit = bit_of(self.place, self.order[stage])
        if self.kinds[stage] == "c":
            mine, other = pl.multiple_of(bit * cols, 128), pl.multiple_of((1 - bit) * cols, 128)
            return rows, (0, pl.ds(mine, cols)), (0, pl.ds(other, cols))
        mine, other = pl.multiple_of(bit * rows, 16), pl.multiple_of((1 - bit) * rows, 16)
        return rows, (mine, pl.ds(0, cols)), (other, pl.ds(0, cols))

    def previous(self, stage):
        return (self.source, self.lo) if stage == 0 else (self.held[stage - 1], 0)

    def reduce_copy(self, stage):
        rows, _, (start, span) = self.halves(stage)
        ref, base = self.previous(stage)
        return pltpu.make_async_remote_copy(
            src_ref=ref.at[pl.ds(base + start, rows), span],
            dst_ref=self.arrive[stage],
            send_sem=self.rs_send.at[stage],
            recv_sem=self.rs_recv.at[stage],
            device_id=across(self.place, self.order[stage]),
            device_id_type=MESH,
        )

    def region(self, pending):
        row, col, rows, cols = self.lo, 0, self.rows, self.cols
        for stage in pending:
            bit = bit_of(self.place, self.order[stage])
            if self.kinds[stage] == "c":
                cols //= 2
                col = col + bit * cols
            else:
                rows //= 2
                row = row + bit * rows
        return pl.ds(pl.multiple_of(row, 16), rows), pl.ds(pl.multiple_of(col, 128), cols)

    def pending(self, stage):
        return sorted(self.gather_order[self.gather_order.index(stage) :])

    def add(self, stage):
        rows, (start, span), _ = self.halves(stage)
        ref, base = self.previous(stage)
        last = stage == len(self.order) - 1
        piece = next(size for size in (128, 96, 80, 64, 48, 32, 16) if rows % size == 0)
        if last:
            row_at, col_at = self.region(range(len(self.order)))

        def one(step, carry):
            at = pl.multiple_of(step * piece, 16)
            total = ref[pl.ds(base + start + at, piece), span].astype(F32) + self.arrive[stage][
                pl.ds(at, piece), :
            ].astype(F32)
            if last:
                self.target[pl.ds(pl.multiple_of(row_at.start + at, 16), piece), col_at] = total.astype(BF)
            else:
                self.held[stage][pl.ds(at, piece), :] = total.astype(BF)
            return carry

        if rows == piece:
            one(0, 0)
        else:
            lax.fori_loop(0, rows // piece, one, 0)

    def gather_copy(self, stage, target=None, sems=None):
        span = (self.target if target is None else target).at[self.region(self.pending(stage))]
        send, recv = (self.ag_send, self.ag_recv) if sems is None else sems
        return pltpu.make_async_remote_copy(
            src_ref=span,
            dst_ref=span,
            send_sem=send.at[stage],
            recv_sem=recv.at[stage],
            device_id=across(self.place, self.order[stage]),
            device_id_type=MESH,
        )


def sum_kinds(count):
    return ["c", "c"] + ["r"] * (count - 2)


def coarse_kinds(count):
    return ["r", "c", "c"] + ["r"] * (count - 3)


def fold_scratch(kinds, rows, cols):
    scratch = []
    for part in rows:
        scratch += Fold.scratch(kinds, part, cols)
    return scratch


def make_folds(place, bits, kinds, parts, refs, cols, wide_first=False):
    count, folds = len(bits), []
    for number, (source, target, rows, lo) in enumerate(parts):
        mine, refs = refs[: 2 * count + 3], refs[2 * count + 3 :]
        folds.append(Fold(place, turned(bits, number), kinds, source, target, lo, rows, cols, mine, wide_first))
    return folds


def cut_parts(source, target, sizes):
    parts, lo = [], 0
    for rows in sizes:
        parts.append((source, target, rows, lo))
        lo += rows
    return parts


def fold_all(folds):
    count = len(folds[0].order)
    for fold in folds:
        fold.reduce_copy(0).start()
    for stage in range(count):
        for fold in folds:
            fold.reduce_copy(stage).wait()
            fold.add(stage)
            if stage + 1 < count:
                fold.reduce_copy(stage + 1).start()
            else:
                fold.gather_copy(fold.gather_order[0]).start()
    for turn in range(count):
        for fold in folds:
            fold.gather_copy(fold.gather_order[turn]).wait()
            if turn + 1 < count:
                fold.gather_copy(fold.gather_order[turn + 1]).start()


def greet(devices):
    barrier = pltpu.get_barrier_semaphore()
    for device in devices:
        pl.semaphore_signal(barrier, inc=1, device_id=device, device_id_type=MESH)
    pl.semaphore_wait(barrier, len(devices))


def split_rows(rows, count, pieces):
    unit = 16 * 2 ** (count - 2)
    units = -(-rows // unit)
    pieces = min(pieces, units)
    sizes = [unit * (units // pieces + (1 if i < units % pieces else 0)) for i in range(pieces)]
    return sizes


def padded(rows, count):
    return sum(split_rows(rows, count, 1))


def block_at(place, sizes, move):
    total = sizes[0] * sizes[1]
    block = lax.rem(place[AXES[0]] * sizes[1] + place[AXES[1]] + (move % total), total)
    return block // sizes[1], lax.rem(block, sizes[1])


def picks(lists_ref, own):
    _, neigh, slots = lists_ref.shape
    listed = lists_ref[0].T
    return jnp.concatenate(
        [one_hot(listed[:, k : k + 1], (slots, own), 1).astype(F32) for k in range(neigh)], axis=0
    ).astype(BF)


def node_math(rows, summed, slope, win_ref, wout_ref, gain):
    pre = product(rows, win_ref[0]) + product(summed, win_ref[1])
    sig = 1.0 / (1.0 + jnp.exp(-pre))
    hidden = (pre * sig).astype(BF)
    normed, inverse = normalize(product(hidden, wout_ref[...]))
    new = (rows.astype(F32) + normed * gain).astype(BF)
    out_slope = normalize_back(slope * gain, normed, inverse).astype(BF)
    swish = sig * (1.0 + pre * (1.0 - sig))
    pre_slope = (outer_cols(out_slope, wout_ref[...]) * swish).astype(BF)
    back = outer_cols(pre_slope, win_ref[1]).astype(BF)
    direct = slope + outer_cols(pre_slope, win_ref[0])
    return new, back, direct, slope * normed, hidden, out_slope, pre_slope


def middle_step(
    bits,
    part_rows,
    factor,
    own_sum,
    coarse_part,
    mesh_ref,
    coarse_ref,
    grad_ref,
    grad_coarse,
    win_ref,
    wout_ref,
    gain_ref,
    new_nodes,
    new_coarse,
    own_slope,
    coarse_slope,
    own_direct,
    coarse_direct,
    pack,
    total,
    all_rows,
    all_sums,
    all_hidden,
    all_out,
    all_pre,
    new_send,
    new_recv,
    slope_send,
    slope_recv,
    *refs,
):
    place = here()
    greet([across(place, bit) for bit in bits])
    count, kinds = len(bits), coarse_kinds(len(bits))
    own, d = mesh_ref.shape
    coarse = coarse_ref.shape[0]
    folds = make_folds(place, bits, kinds, cut_parts(coarse_part, total, part_rows), refs, d, True)
    for fold in folds:
        fold.reduce_copy(0).start()
    gain = gain_ref[...]
    gains = [jnp.zeros((1, d), F32)]
    coarse_direct[...] = jnp.zeros_like(coarse_direct)
    pieces = 4 if own % 64 == 0 else 1
    piece = own // pieces

    def own_piece(number):
        span = pl.ds(number * piece, piece)
        results = node_math(
            mesh_ref[span, :], own_sum[span, :], grad_ref[span, :].astype(F32), win_ref, wout_ref, gain
        )
        new_nodes[span, :], own_slope[span, :], own_direct[span, :] = results[:3]
        gains.append(jnp.sum(results[3], axis=0, keepdims=True))
        all_rows[span, :], all_sums[span, :] = mesh_ref[span, :], own_sum[span, :]
        all_hidden[span, :], all_out[span, :], all_pre[span, :] = results[4:]

    todo = list(range(pieces))
    for stage in range(count):
        if todo:
            own_piece(todo.pop(0))
        for fold in folds:
            fold.reduce_copy(stage).wait()
            fold.add(stage)
            if stage + 1 < count:
                fold.reduce_copy(stage + 1).start()
            else:
                fold.gather_copy(fold.gather_order[0]).start()
    while todo:
        own_piece(todo.pop(0))
    wide = kinds.count("c")
    for turn in range(wide):
        for fold in folds:
            fold.gather_copy(fold.gather_order[turn]).wait()
            if turn + 1 < wide:
                fold.gather_copy(fold.gather_order[turn + 1]).start()
    spans, shares = [], []
    for fold in folds:
        span, _ = fold.region(fold.pending(fold.gather_order[wide]))
        first = 1
        for stage in range(count):
            if kinds[stage] == "c":
                first = first * (1 - bit_of(place, fold.order[stage]))
        spans.append(span)
        shares.append(jnp.full((span.size, 1), first, jnp.int32).astype(F32))
    share = jnp.concatenate(shares, axis=0)
    rows = jnp.concatenate([coarse_ref[span, :] for span in spans], axis=0)
    summed = jnp.concatenate([total[span, :] for span in spans], axis=0)
    slope = jnp.concatenate([grad_coarse[span, :] for span in spans], axis=0).astype(F32)
    new, back, direct, gain_term, hidden, out_slope, pre_slope = node_math(
        rows, summed, slope, win_ref, wout_ref, gain
    )
    direct = direct * share
    at = 0
    for number, (fold, span) in enumerate(zip(folds, spans)):
        here_rows = slice(at, at + span.size)
        new_coarse[span, :], coarse_slope[span, :] = new[here_rows], back[here_rows]
        coarse_direct[span, :] = direct[here_rows]
        at += span.size
    tail = range(wide, count)

    def tail_copies(number, fold, turn):
        stage = fold.gather_order[turn]
        return (
            fold.gather_copy(stage, coarse_slope, (slope_send.at[number], slope_recv.at[number])),
            fold.gather_copy(stage, new_coarse, (new_send.at[number], new_recv.at[number])),
        )

    for number, fold in enumerate(folds):
        for copy in tail_copies(number, fold, wide):
            copy.start()
    span = pl.ds(own, at)
    all_rows[span, :], all_sums[span, :] = rows, summed
    all_hidden[span, :] = (hidden.astype(F32) * share).astype(BF)
    all_out[span, :] = out_slope
    all_pre[span, :] = (pre_slope.astype(F32) * share).astype(BF)
    gains.append(jnp.sum(gain_term * share, axis=0, keepdims=True))
    jobs = [
        lambda: (0, inner_rows(all_rows[...], all_pre[...])),
        lambda: (d, inner_rows(all_sums[...], all_pre[...])),
        lambda: (2 * d, inner_rows(all_hidden[...], all_out[...])),
    ]
    for turn in tail:
        if jobs:
            lo, result = jobs.pop(0)()
            pack[pl.ds(lo, d), :] = (result * factor).astype(BF)
        for number, fold in enumerate(folds):
            for copy in tail_copies(number, fold, turn):
                copy.wait()
            if turn + 1 < count:
                for copy in tail_copies(number, fold, turn + 1):
                    copy.start()
    assert not jobs
    rest = pack.shape[0] - 3 * d
    pack[pl.ds(3 * d, rest), :] = jnp.broadcast_to(sum(gains) * factor, (rest, d)).astype(BF)


def final_step(
    bits,
    sizes,
    moves,
    edge_cuts,
    node_cuts,
    edge_ref,
    node_ref,
    term_ref,
    lists_ref,
    direct_ref,
    edge_out,
    node_out,
    nodes_grad,
    landed,
    send,
    recv,
    *refs,
):
    place = here()
    greet([across(place, bit) for bit in bits] + [block_at(place, sizes, -move) for move in moves])
    copies = []
    for k, move in enumerate(moves):
        copy = pltpu.make_async_remote_copy(
            src_ref=term_ref.at[k],
            dst_ref=landed.at[k],
            send_sem=send.at[k],
            recv_sem=recv.at[k],
            device_id=block_at(place, sizes, move),
            device_id_type=MESH,
        )
        copy.start()
        copies.append(copy)
    cols = edge_ref.shape[1]
    parts = cut_parts(edge_ref, edge_out, edge_cuts) + cut_parts(node_ref, node_out, node_cuts)
    fold_all(make_folds(place, bits, sum_kinds(len(bits)), parts, refs, cols))
    for copy in copies:
        copy.wait()
    own = direct_ref.shape[0]
    back = landed[...].reshape(landed.shape[0] * landed.shape[1], cols)
    nodes_grad[...] = (direct_ref[...] + inner_rows(picks(lists_ref, own), back)).astype(BF)


def edge_index(tiles_ref, own, halo):
    count, _, width = tiles_ref.shape
    flat = tiles_ref[...].reshape(2 * count, width)
    fine = jnp.where(flat < own, flat, flat + halo)
    row = lax.broadcasted_iota(jnp.int32, flat.shape, 0)
    flat = jnp.where(lax.rem(row, 2) == 0, flat, fine)
    turned_flat = flat.T
    send_col = jnp.concatenate([turned_flat[:, 2 * t : 2 * t + 1] for t in range(count)], axis=0)
    recv_col = jnp.concatenate([turned_flat[:, 2 * t + 1 : 2 * t + 2] for t in range(count)], axis=0)
    send_row = jnp.concatenate([flat[2 * t : 2 * t + 1, :] for t in range(count)], axis=1)
    recv_row = jnp.concatenate([flat[2 * t + 1 : 2 * t + 2, :] for t in range(count)], axis=1)
    return send_col, recv_col, send_row, recv_row


def edge_forward(
    tile_width,
    sizes,
    moves,
    live_ref,
    lat_ref,
    tiles_ref,
    lists_ref,
    mesh_ref,
    coarse_ref,
    win_ref,
    wout_ref,
    gain_ref,
    new_ref,
    hid_ref,
    slope_ref,
    norm_ref,
    inv_ref,
    agg_own,
    agg_coarse,
    halo_ref,
    proj_s,
    proj_r,
    agg,
    leaving,
    landed,
    send,
    recv,
):
    step = pl.program_id(0)
    own, halo = mesh_ref.shape[0], halo_ref.shape[0]
    rows = agg.shape[0]
    block = lat_ref.shape[0]

    @pl.when(step == 0)
    def _():
        place = here()
        greet([block_at(place, sizes, move) for move in moves])
        slots = leaving.shape[1]
        rows_out = product(picks(lists_ref, own), mesh_ref[...]).astype(BF)
        copies = []
        for k, move in enumerate(moves):
            leaving[k] = rows_out[k * slots : (k + 1) * slots]
        for k, move in enumerate(moves):
            copy = pltpu.make_async_remote_copy(
                src_ref=leaving.at[k],
                dst_ref=landed.at[k],
                send_sem=send.at[k],
                recv_sem=recv.at[k],
                device_id=block_at(place, sizes, -move),
                device_id_type=MESH,
            )
            copy.start()
            copies.append(copy)
        agg[...] = jnp.zeros_like(agg)

        def project(part, lo):
            span = pl.ds(lo, part.shape[0])
            proj_s[span, :] = product(part, win_ref[1]).astype(BF)
            proj_r[span, :] = product(part, win_ref[2]).astype(BF)

        project(mesh_ref[...], 0)
        project(coarse_ref[...], own + halo)
        for copy in copies:
            copy.wait()
        halo_ref[...] = landed[...].reshape(halo_ref.shape)
        project(halo_ref[...], own)

    send_col, recv_col, _, recv_row = edge_index(tiles_ref, own, halo)
    rows_in = lat_ref[...]
    pre = (
        product(rows_in, win_ref[0])
        + product(one_hot(send_col, (block, rows), 1), proj_s[...])
        + product(one_hot(recv_col, (block, rows), 1), proj_r[...])
    )
    sig = 1.0 / (1.0 + jnp.exp(-pre))
    hidden = (pre * sig).astype(BF)
    slope_ref[...] = (sig * (1.0 + pre * (1.0 - sig))).astype(BF)
    hid_ref[...] = hidden
    normed, inverse = normalize(product(hidden, wout_ref[...]))
    norm_ref[...] = normed.astype(BF)
    inv_ref[...] = inverse
    place = step * block + lax.broadcasted_iota(jnp.int32, (block, 1), 0)
    alive = jnp.where(place < live_ref[0] * tile_width, 1.0, 0.0)
    message = normed * gain_ref[...] * alive
    new_ref[...] = (rows_in.astype(F32) + message).astype(BF)
    agg[...] += product(one_hot(recv_row, (rows, block), 0), message.astype(BF))

    @pl.when(step == pl.num_programs(0) - 1)
    def _():
        agg_own[...] = agg[pl.ds(0, own), :].astype(BF)
        agg_coarse[...] = agg[pl.ds(own + halo, rows - own - halo), :].astype(BF)


def edge_backward(
    tile_width,
    factor,
    live_ref,
    lat_ref,
    grad_ref,
    hid_ref,
    slope_ref,
    norm_ref,
    inv_ref,
    tiles_ref,
    mesh_ref,
    halo_ref,
    coarse_ref,
    own_slope,
    coarse_slope,
    own_direct,
    coarse_direct,
    win_ref,
    wout_ref,
    gain_ref,
    edges_grad,
    pack,
    own_term,
    halo_term,
    table,
    sent,
    received,
    first_acc,
    out_acc,
    gain_grad,
):
    step = pl.program_id(0)
    own, halo = mesh_ref.shape[0], halo_ref.shape[0]
    rows = table.shape[0]
    block = lat_ref.shape[0]

    @pl.when(step == 0)
    def _():
        for acc in (sent, received, first_acc, out_acc, gain_grad):
            acc[...] = jnp.zeros_like(acc)
        table[pl.ds(0, own), :] = own_slope[...]
        table[pl.ds(own, halo), :] = jnp.zeros((halo, table.shape[1]), BF)
        table[pl.ds(own + halo, rows - own - halo), :] = coarse_slope[...]

    _, recv_col, send_row, recv_row = edge_index(tiles_ref, own, halo)
    place = step * block + lax.broadcasted_iota(jnp.int32, (block, 1), 0)
    alive = jnp.where(place < live_ref[0] * tile_width, 1.0, 0.0)
    edge_slope = grad_ref[...].astype(F32)
    message_slope = (
        edge_slope + product(one_hot(recv_col, (block, rows), 1), table[...])
    ) * alive
    normed = norm_ref[...].astype(F32)
    gain_grad[...] += jnp.sum(message_slope * normed, axis=0, keepdims=True)
    out_slope = normalize_back(message_slope * gain_ref[...], normed, inv_ref[...]).astype(BF)
    out_acc[...] += inner_rows(hid_ref[...], out_slope)
    pre_slope = (outer_cols(out_slope, wout_ref[...]) * slope_ref[...].astype(F32)).astype(BF)
    edges_grad[...] = (edge_slope + outer_cols(pre_slope, win_ref[0])).astype(BF)
    first_acc[...] += inner_rows(lat_ref[...], pre_slope)
    sent[...] += product(one_hot(send_row, (rows, block), 0), pre_slope)
    received[...] += product(one_hot(recv_row, (rows, block), 0), pre_slope)

    @pl.when(step == pl.num_programs(0) - 1)
    def _():
        d = first_acc.shape[0]
        coarse = coarse_ref.shape[0]
        pack[pl.ds(0, d), :] = (first_acc[...] * factor).astype(BF)
        pack[pl.ds(3 * d, d), :] = (out_acc[...] * factor).astype(BF)
        sums = [None, None]
        for part, lo in ((mesh_ref, 0), (halo_ref, own), (coarse_ref, own + halo)):
            span = pl.ds(lo, part.shape[0])
            total = None
            for which, source in enumerate((sent, received)):
                piece = source[span, :].astype(BF)
                weight = inner_rows(part[...], piece)
                sums[which] = weight if sums[which] is None else sums[which] + weight
                back = outer_cols(piece, win_ref[1 + which])
                total = back if total is None else total + back
            if part is mesh_ref:
                own_term[...] = total + own_direct[...]
            elif part is halo_ref:
                halo_term[...] = total.astype(BF)
            else:
                pack[pl.ds(4 * d, coarse), :] = (total + coarse_direct[...]).astype(BF)
        pack[pl.ds(d, d), :] = (sums[0] * factor).astype(BF)
        pack[pl.ds(2 * d, d), :] = (sums[1] * factor).astype(BF)
        rest = pack.shape[0] - 4 * d - coarse
        pack[pl.ds(4 * d + coarse, rest), :] = jnp.broadcast_to(gain_grad[...] * factor, (rest, d)).astype(BF)


def whole(shape):
    zero = (0,) * len(shape)
    return pl.BlockSpec(shape, lambda i: zero)


def by_rows(block, width):
    return pl.BlockSpec((block, width), lambda i: (i, 0))


def by_cols(block):
    return pl.BlockSpec((1, block), lambda i: (0, i))


def shape_of(shape, dtype):
    return jax.ShapeDtypeStruct(shape, dtype)


def cost(flops, moved):
    return pl.CostEstimate(flops=int(flops), bytes_accessed=int(moved), transcendentals=0)


PARAMS = dict(
    compiler_params=pltpu.CompilerParams(
        dimension_semantics=("arbitrary",), vmem_limit_bytes=60 * 1024 * 1024
    )
)


def talking(number, grid=False):
    return pltpu.CompilerParams(
        collective_id=number,
        has_side_effects=True,
        vmem_limit_bytes=60 * 1024 * 1024,
        dimension_semantics=("arbitrary",) if grid else None,
    )


def on_device(
    mesh_nodes,
    coarse_nodes,
    edge_latents,
    edge_tiles,
    send_lists,
    tiles_live,
    edge_in,
    edge_out,
    edge_gain,
    node_in,
    node_out,
    node_gain,
    grad_nodes,
    grad_coarse,
    grad_edges,
):
    sizes = tuple(lax.axis_size(axis) for axis in AXES)
    block_count = sizes[0] * sizes[1]
    bits = square_bits(sizes)
    count = len(bits)
    own, d = mesh_nodes.shape
    neigh, slots = send_lists.shape[1:]
    coarse = coarse_nodes.shape[0]
    halo = neigh * slots
    rows = own + halo + coarse
    tile_dev, _, tile_width = edge_tiles.shape
    edges = tile_dev * tile_width
    tiles = 4 if tile_dev % 4 == 0 else 1
    block = tiles * tile_width
    moves = cycle_moves(neigh, block_count)
    factor = float(edges * block_count) ** (-0.5)
    e_gain, n_gain = edge_gain.reshape(1, d), node_gain.reshape(1, d)
    vmem = pl.BlockSpec(memory_space=pltpu.VMEM)
    smem = pl.BlockSpec(memory_space=pltpu.SMEM)
    wide, col = by_rows(block, d), by_rows(block, 1)
    pairs = pl.BlockSpec((tiles, 2, tile_width), lambda i: (i, 0, 0))
    tables = [whole((own, d)), whole((halo, d)), whole((coarse, d))]
    weights = [whole((3, d, d)), whole((d, d)), whole((1, d))]
    swap = [pltpu.VMEM((neigh, slots, d), BF)] * 2 + [pltpu.SemaphoreType.DMA((neigh,))] * 2
    new_edges, hidden, slope, normed, inverse, agg_own, agg_coarse, incoming = pl.pallas_call(
        functools.partial(edge_forward, tile_width, sizes, moves),
        grid=(edges // block,),
        in_specs=[smem, wide, pairs, whole((1, neigh, slots)), tables[0], tables[2]] + weights,
        out_specs=[wide] * 4 + [col, tables[0], tables[2], tables[1]],
        out_shape=[shape_of((edges, d), BF)] * 4
        + [
            shape_of((edges, 1), F32),
            shape_of((own, d), BF),
            shape_of((coarse, d), BF),
            shape_of((halo, d), BF),
        ],
        scratch_shapes=[
            pltpu.VMEM((rows, d), BF),
            pltpu.VMEM((rows, d), BF),
            pltpu.VMEM((rows, d), F32),
        ]
        + swap,
        cost_estimate=cost(2 * edges * d * (3 * rows + 2 * d), 12 * edges * d),
        compiler_params=talking(0, grid=True),
    )(
        tiles_live, edge_latents, edge_tiles, send_lists, mesh_nodes, coarse_nodes, edge_in, edge_out, e_gain
    )
    sum_rows = padded(coarse, count)
    grown = [agg_coarse, coarse_nodes, grad_coarse]
    if sum_rows > coarse:
        grown = [jnp.pad(array, ((0, sum_rows - coarse), (0, 0))) for array in grown]
    coarse_rows = split_rows(sum_rows, count, 3)
    all_rows = own + sum_rows // 2 ** (count - 2)
    node_rows = padded(3 * d + 1, count)
    parts = len(coarse_rows)
    new_nodes, new_coarse, own_slope, c_slope, own_direct, c_direct, node_pack = pl.pallas_call(
        functools.partial(middle_step, bits, coarse_rows, factor),
        in_specs=[vmem] * 9,
        out_specs=[vmem] * 7,
        out_shape=[
            shape_of((own, d), BF),
            shape_of((sum_rows, d), BF),
            shape_of((own, d), BF),
            shape_of((sum_rows, d), BF),
            shape_of((own, d), F32),
            shape_of((sum_rows, d), F32),
            shape_of((node_rows, d), BF),
        ],
        scratch_shapes=[pltpu.VMEM((sum_rows, d), BF)]
        + [pltpu.VMEM((all_rows, d), BF)] * 5
        + [pltpu.SemaphoreType.DMA((parts, count))] * 4
        + fold_scratch(coarse_kinds(count), coarse_rows, d),
        compiler_params=talking(1),
    )(agg_own, grown[0], mesh_nodes, grown[1], grad_nodes, grown[2], node_in, node_out, n_gain)
    if sum_rows > coarse:
        new_coarse, c_slope, c_direct = (array[:coarse] for array in (new_coarse, c_slope, c_direct))
    edge_rows = padded(4 * d + coarse + 1, count)
    edges_grad, edge_pack, own_term, halo_term = pl.pallas_call(
        functools.partial(edge_backward, tile_width, factor),
        grid=(edges // block,),
        in_specs=[smem] + [wide] * 5 + [col, pairs] + tables
        + [whole((own, d)), whole((coarse, d))] * 2 + weights,
        out_specs=[wide, whole((edge_rows, d)), whole((own, d)), whole((halo, d))],
        out_shape=[
            shape_of((edges, d), BF),
            shape_of((edge_rows, d), BF),
            shape_of((own, d), F32),
            shape_of((halo, d), BF),
        ],
        scratch_shapes=[
            pltpu.VMEM((rows, d), BF),
            pltpu.VMEM((rows, d), F32),
            pltpu.VMEM((rows, d), F32),
            pltpu.VMEM((d, d), F32),
            pltpu.VMEM((d, d), F32),
            pltpu.VMEM((1, d), F32),
        ],
        cost_estimate=cost(2 * edges * d * (3 * rows + 4 * d), 14 * edges * d),
        **PARAMS,
    )(
        tiles_live, edge_latents, grad_edges, hidden, slope, normed, inverse, edge_tiles, mesh_nodes, incoming,
        coarse_nodes, own_slope, c_slope, own_direct, c_direct, edge_in, edge_out, e_gain,
    )
    edge_cuts, node_cuts = split_rows(edge_rows, count, 6), split_rows(node_rows, count, 3)
    edge_sum, node_sum, nodes_grad = pl.pallas_call(
        functools.partial(final_step, bits, sizes, moves, edge_cuts, node_cuts),
        in_specs=[vmem] * 5,
        out_specs=[vmem] * 3,
        out_shape=[shape_of((edge_rows, d), BF), shape_of((node_rows, d), BF), shape_of((own, d), BF)],
        scratch_shapes=swap[1:] + fold_scratch(sum_kinds(count), edge_cuts + node_cuts, d),
        compiler_params=talking(2),
    )(edge_pack, node_pack, halo_term.reshape(neigh, slots, d), send_lists, own_term)
    return (
        new_nodes,
        new_coarse,
        new_edges,
        nodes_grad,
        edge_sum[4 * d : 4 * d + coarse],
        edges_grad,
        edge_sum[: 3 * d].reshape(3, d, d),
        edge_sum[3 * d : 4 * d],
        edge_sum[4 * d + coarse].astype(F32),
        node_sum[: 2 * d].reshape(2, d, d),
        node_sum[2 * d : 3 * d],
        node_sum[3 * d].astype(F32),
    )


def solution(mesh):
    rows2 = P(AXES, None)
    rows3 = P(AXES, None, None)
    in_specs = (
        rows2, P(), rows2, rows3, rows3, P(AXES), P(), P(), P(), P(), P(), P(), rows2, P(), rows2,
    )
    out_specs = (rows2, P(), rows2, rows2, P(), rows2, P(), P(), P(), P(), P(), P())
    return jax.shard_map(
        on_device, mesh=mesh, in_specs=in_specs, out_specs=out_specs, check_vma=False
    )
```

```python
import functools

import jax
import jax.numpy as jnp
from jax import lax
from jax.experimental import pallas as pl
from jax.experimental.pallas import tpu as pltpu
from jax.sharding import PartitionSpec as P

EPS = 1e-05
BF = jnp.bfloat16
F32 = jnp.float32
AXES = ("lat", "blk")
MESH = pl.DeviceIdType.MESH


def dims(a, b, ca, cb):
    return lax.dot_general(a, b, (((ca,), (cb,)), ((), ())), preferred_element_type=F32)


def product(a, b):
    return dims(a, b, 1, 0)


def inner_rows(a, b):
    return dims(a, b, 0, 0)


def outer_cols(a, b):
    return dims(a, b, 1, 1)


def normalize(values):
    centered = values - jnp.mean(values, axis=-1, keepdims=True)
    inverse = lax.rsqrt(jnp.mean(centered * centered, axis=-1, keepdims=True) + EPS)
    return (centered * inverse, inverse)


def normalize_back(upstream, normed, inverse):
    return inverse * (
        upstream
        - jnp.mean(upstream, axis=-1, keepdims=True)
        - normed * jnp.mean(upstream * normed, axis=-1, keepdims=True)
    )


def one_hot(index, shape, axis):
    return jnp.where(lax.broadcasted_iota(jnp.int32, shape, axis) == index, 1.0, 0.0).astype(BF)


def cycle_moves(neigh_count, block_count):
    near_count = neigh_count // 2 - 1
    near = [position - near_count for position in range(near_count)] + [
        position + 1 for position in range(near_count)
    ]
    return near + [block_count // 4, block_count // 2]


def square_bits(sizes):
    found = []
    for axis, size in zip(AXES, sizes):
        step = 1
        while step < size:
            found.append((axis, step))
            step *= 2
        assert step == size
    return found


def turned(bits, turn):
    middle = bits[1:-1]
    turn = turn % len(middle)
    return [bits[0]] + middle[turn:] + middle[:turn] + [bits[-1]]


def bit_of(place, bit):
    return lax.rem(place[bit[0]] // bit[1], 2)


def across(place, bit):
    axis, step = bit
    moved = dict(place)
    moved[axis] = place[axis] + step - 2 * step * bit_of(place, bit)
    return tuple(moved[axis] for axis in AXES)


def here():
    return {axis: lax.axis_index(axis) for axis in AXES}


class Fold:
    def __init__(self, place, order, kinds, source, target, lo, rows, cols, refs, wide_first=False):
        count = len(order)
        self.place, self.order, self.kinds = place, order, kinds
        self.source, self.target, self.lo = source, target, lo
        self.rows, self.cols = rows, cols
        self.arrive, self.held = refs[:count], refs[count : 2 * count - 1]
        if refs:
            self.rs_send, self.rs_recv, self.ag_send, self.ag_recv = refs[2 * count - 1 :]
        self.sizes = Fold.shapes(kinds, rows, cols)
        self.gather_order = list(reversed(range(count)))
        if wide_first:
            self.gather_order.sort(key=lambda stage: kinds[stage] == "r")

    @staticmethod
    def shapes(kinds, rows, cols):
        found = []
        for kind in kinds:
            if kind == "c":
                cols //= 2
            else:
                rows //= 2
            found.append((rows, cols))
        return found

    @staticmethod
    def scratch(kinds, rows, cols):
        shapes, count = Fold.shapes(kinds, rows, cols), len(kinds)
        return (
            [pltpu.VMEM(shape, BF) for shape in shapes]
            + [pltpu.VMEM(shape, BF) for shape in shapes[:-1]]
            + [pltpu.SemaphoreType.DMA((count,))] * 4
        )

    def halves(self, stage):
        rows, cols = self.sizes[stage]
        bit = bit_of(self.place, self.order[stage])
        if self.kinds[stage] == "c":
            mine, other = pl.multiple_of(bit * cols, 128), pl.multiple_of((1 - bit) * cols, 128)
            return rows, (0, pl.ds(mine, cols)), (0, pl.ds(other, cols))
        mine, other = pl.multiple_of(bit * rows, 16), pl.multiple_of((1 - bit) * rows, 16)
        return rows, (mine, pl.ds(0, cols)), (other, pl.ds(0, cols))

    def previous(self, stage):
        return (self.source, self.lo) if stage == 0 else (self.held[stage - 1], 0)

    def reduce_copy(self, stage):
        rows, _, (start, span) = self.halves(stage)
        ref, base = self.previous(stage)
        return pltpu.make_async_remote_copy(
            src_ref=ref.at[pl.ds(base + start, rows), span],
            dst_ref=self.arrive[stage],
            send_sem=self.rs_send.at[stage],
            recv_sem=self.rs_recv.at[stage],
            device_id=across(self.place, self.order[stage]),
            device_id_type=MESH,
        )

    def region(self, pending):
        row, col, rows, cols = self.lo, 0, self.rows, self.cols
        for stage in pending:
            bit = bit_of(self.place, self.order[stage])
            if self.kinds[stage] == "c":
                cols //= 2
                col = col + bit * cols
            else:
                rows //= 2
                row = row + bit * rows
        return pl.ds(pl.multiple_of(row, 16), rows), pl.ds(pl.multiple_of(col, 128), cols)

    def pending(self, stage):
        return sorted(self.gather_order[self.gather_order.index(stage) :])

    def add(self, stage):
        rows, (start, span), _ = self.halves(stage)
        ref, base = self.previous(stage)
        last = stage == len(self.order) - 1
        piece = next(size for size in (128, 96, 80, 64, 48, 32, 16) if rows % size == 0)
        if last:
            row_at, col_at = self.region(range(len(self.order)))

        def one(step, carry):
            at = pl.multiple_of(step * piece, 16)
            total = ref[pl.ds(base + start + at, piece), span].astype(F32) + self.arrive[stage][
                pl.ds(at, piece), :
            ].astype(F32)
            if last:
                self.target[pl.ds(pl.multiple_of(row_at.start + at, 16), piece), col_at] = total.astype(BF)
            else:
                self.held[stage][pl.ds(at, piece), :] = total.astype(BF)
            return carry

        if rows == piece:
            one(0, 0)
        else:
            lax.fori_loop(0, rows // piece, one, 0)

    def gather_copy(self, stage, target=None, sems=None):
        span = (self.target if target is None else target).at[self.region(self.pending(stage))]
        send, recv = (self.ag_send, self.ag_recv) if sems is None else sems
        return pltpu.make_async_remote_copy(
            src_ref=span,
            dst_ref=span,
            send_sem=send.at[stage],
            recv_sem=recv.at[stage],
            device_id=across(self.place, self.order[stage]),
            device_id_type=MESH,
        )


    def delivery(self):
        span = pl.ds(self.lo, self.rows)
        return pltpu.make_async_copy(self.target.at[span, :], self.out.at[span, :], self.out_sem)

    def deliver(self):
        self.delivery().start()

    def begin(self, turn):
        count = len(self.order)
        if turn < count:
            self.reduce_copy(turn).start()
        elif turn < 2 * count:
            self.gather_copy(self.gather_order[turn - count]).start()

    def advance(self, turn):
        count = len(self.order)
        if turn < count:
            self.reduce_copy(turn).wait()
            self.add(turn)
        else:
            self.gather_copy(self.gather_order[turn - count]).wait()
        self.begin(turn + 1)


def sum_kinds(count):
    return ["c", "c"] + ["r"] * (count - 2)


def coarse_kinds(count):
    return ["r", "c", "c"] + ["r"] * (count - 3)


def fold_scratch(kinds, rows, cols):
    scratch = []
    for part in rows:
        scratch += Fold.scratch(kinds, part, cols)
    return scratch


def make_folds(place, bits, kinds, parts, refs, cols, wide_first=False):
    count, folds = len(bits), []
    for number, (source, target, rows, lo) in enumerate(parts):
        mine, refs = refs[: 2 * count + 3], refs[2 * count + 3 :]
        order = turned(bits, number)
        folds.append(Fold(place, order, kinds, source, target, lo, rows, cols, mine, wide_first))
    return folds


def cut_parts(source, target, sizes):
    parts, lo = [], 0
    for rows in sizes:
        parts.append((source, target, rows, lo))
        lo += rows
    return parts


def greet(devices):
    barrier = pltpu.get_barrier_semaphore()
    for device in devices:
        pl.semaphore_signal(barrier, inc=1, device_id=device, device_id_type=MESH)
    pl.semaphore_wait(barrier, len(devices))


def split_rows(rows, count, pieces):
    unit = 16 * 2 ** (count - 2)
    units = -(-rows // unit)
    pieces = min(pieces, units)
    sizes = [unit * (units // pieces + (1 if i < units % pieces else 0)) for i in range(pieces)]
    return sizes


def padded(rows, count):
    return sum(split_rows(rows, count, 1))


def block_at(place, sizes, move):
    total = sizes[0] * sizes[1]
    block = lax.rem(place[AXES[0]] * sizes[1] + place[AXES[1]] + (move % total), total)
    return block // sizes[1], lax.rem(block, sizes[1])


def picks(lists_ref, own):
    _, neigh, slots = lists_ref.shape
    listed = lists_ref[0].T
    return jnp.concatenate(
        [one_hot(listed[:, k : k + 1], (slots, own), 1).astype(F32) for k in range(neigh)], axis=0
    ).astype(BF)


def node_math(rows, summed, slope, win_ref, wout_ref, gain):
    pre = product(rows, win_ref[0]) + product(summed, win_ref[1])
    sig = 1.0 / (1.0 + jnp.exp(-pre))
    hidden = (pre * sig).astype(BF)
    normed, inverse = normalize(product(hidden, wout_ref[...]))
    new = (rows.astype(F32) + normed * gain).astype(BF)
    out_slope = normalize_back(slope * gain, normed, inverse).astype(BF)
    swish = sig * (1.0 + pre * (1.0 - sig))
    pre_slope = (outer_cols(out_slope, wout_ref[...]) * swish).astype(BF)
    back = outer_cols(pre_slope, win_ref[1]).astype(BF)
    direct = slope + outer_cols(pre_slope, win_ref[0])
    return new, back, direct, slope * normed, hidden, out_slope, pre_slope


def middle_step(
    bits,
    part_rows,
    factor,
    own_sum,
    coarse_part,
    mesh_ref,
    coarse_ref,
    grad_ref,
    grad_coarse,
    win_ref,
    wout_ref,
    gain_ref,
    new_nodes,
    new_part,
    own_slope,
    coarse_slope,
    own_direct,
    direct_part,
    pack,
    node_gain,
    total,
    all_rows,
    all_sums,
    all_hidden,
    all_out,
    all_pre,
    slope_send,
    slope_recv,
    *refs,
):
    place = here()
    greet([across(place, bit) for bit in bits])
    count, kinds = len(bits), coarse_kinds(len(bits))
    own, d = mesh_ref.shape
    coarse = coarse_ref.shape[0]
    folds = make_folds(place, bits, kinds, cut_parts(coarse_part, total, part_rows), refs, d, True)
    for fold in folds:
        fold.reduce_copy(0).start()
    gain = gain_ref[...]
    gains = [jnp.zeros((1, d), F32)]
    pieces = 4 if own % 64 == 0 else 1
    piece = own // pieces

    def own_piece(number):
        span = pl.ds(number * piece, piece)
        results = node_math(
            mesh_ref[span, :], own_sum[span, :], grad_ref[span, :].astype(F32), win_ref, wout_ref, gain
        )
        new_nodes[span, :], own_slope[span, :], own_direct[span, :] = results[:3]
        gains.append(jnp.sum(results[3], axis=0, keepdims=True))
        all_rows[span, :], all_sums[span, :] = mesh_ref[span, :], own_sum[span, :]
        all_hidden[span, :], all_out[span, :], all_pre[span, :] = results[4:]

    todo = list(range(pieces))
    for stage in range(count):
        if todo:
            own_piece(todo.pop(0))
        for fold in folds:
            fold.reduce_copy(stage).wait()
            fold.add(stage)
            if stage + 1 < count:
                fold.reduce_copy(stage + 1).start()
            else:
                fold.gather_copy(fold.gather_order[0]).start()
    while todo:
        own_piece(todo.pop(0))
    wide = kinds.count("c")
    for turn in range(wide):
        for fold in folds:
            fold.gather_copy(fold.gather_order[turn]).wait()
            if turn + 1 < wide:
                fold.gather_copy(fold.gather_order[turn + 1]).start()
    spans, shares = [], []
    for fold in folds:
        span, _ = fold.region(fold.pending(fold.gather_order[wide]))
        first = 1
        for stage in range(count):
            if kinds[stage] == "c":
                first = first * (1 - bit_of(place, fold.order[stage]))
        spans.append(span)
        shares.append(jnp.full((span.size, 1), first, jnp.int32).astype(F32))
    share = jnp.concatenate(shares, axis=0)
    rows = jnp.concatenate([coarse_ref[span, :] for span in spans], axis=0)
    summed = jnp.concatenate([total[span, :] for span in spans], axis=0)
    slope = jnp.concatenate([grad_coarse[span, :] for span in spans], axis=0).astype(F32)
    new, back, direct, gain_term, hidden, out_slope, pre_slope = node_math(
        rows, summed, slope, win_ref, wout_ref, gain
    )
    new_part[...] = new
    direct_part[...] = direct * share
    at = 0
    for fold, span in zip(folds, spans):
        coarse_slope[span, :] = back[at : at + span.size]
        at += span.size
    tail = range(wide, count)

    def tail_copy(number, fold, turn):
        stage = fold.gather_order[turn]
        return fold.gather_copy(stage, coarse_slope, (slope_send.at[number], slope_recv.at[number]))

    for number, fold in enumerate(folds):
        tail_copy(number, fold, wide).start()
    span = pl.ds(own, at)
    all_rows[span, :], all_sums[span, :] = rows, summed
    all_hidden[span, :] = (hidden.astype(F32) * share).astype(BF)
    all_out[span, :] = out_slope
    all_pre[span, :] = (pre_slope.astype(F32) * share).astype(BF)
    gains.append(jnp.sum(gain_term * share, axis=0, keepdims=True))
    jobs = [
        lambda: (0, inner_rows(all_rows[...], all_pre[...])),
        lambda: (d, inner_rows(all_sums[...], all_pre[...])),
        lambda: (2 * d, inner_rows(all_hidden[...], all_out[...])),
    ]
    for turn in tail:
        if jobs:
            lo, result = jobs.pop(0)()
            pack[pl.ds(lo, d), :] = (result * factor).astype(BF)
        for number, fold in enumerate(folds):
            tail_copy(number, fold, turn).wait()
            if turn + 1 < count:
                tail_copy(number, fold, turn + 1).start()
    assert not jobs
    node_gain[...] = sum(gains)


def edge_index(tiles_ref, own, halo):
    count, _, width = tiles_ref.shape
    flat = tiles_ref[...].reshape(2 * count, width)
    fine = jnp.where(flat < own, flat, flat + halo)
    row = lax.broadcasted_iota(jnp.int32, flat.shape, 0)
    flat = jnp.where(lax.rem(row, 2) == 0, flat, fine)
    turned_flat = flat.T
    send_col = jnp.concatenate([turned_flat[:, 2 * t : 2 * t + 1] for t in range(count)], axis=0)
    recv_col = jnp.concatenate([turned_flat[:, 2 * t + 1 : 2 * t + 2] for t in range(count)], axis=0)
    send_row = jnp.concatenate([flat[2 * t : 2 * t + 1, :] for t in range(count)], axis=1)
    recv_row = jnp.concatenate([flat[2 * t + 1 : 2 * t + 2, :] for t in range(count)], axis=1)
    return send_col, recv_col, send_row, recv_row


def edge_forward(
    tile_width,
    sizes,
    moves,
    live_ref,
    lat_ref,
    tiles_ref,
    lists_ref,
    mesh_ref,
    coarse_ref,
    win_ref,
    wout_ref,
    gain_ref,
    new_ref,
    hid_ref,
    slope_ref,
    norm_ref,
    inv_ref,
    agg_own,
    agg_coarse,
    halo_ref,
    proj_s,
    proj_r,
    agg,
    leaving,
    landed,
    send,
    recv,
):
    step = pl.program_id(0)
    own, halo = mesh_ref.shape[0], halo_ref.shape[0]
    rows = agg.shape[0]
    block = lat_ref.shape[0]

    @pl.when(step == 0)
    def _():
        place = here()
        greet([block_at(place, sizes, move) for move in moves])
        slots = leaving.shape[1]
        rows_out = product(picks(lists_ref, own), mesh_ref[...]).astype(BF)
        copies = []
        for k, move in enumerate(moves):
            leaving[k] = rows_out[k * slots : (k + 1) * slots]
        for k, move in enumerate(moves):
            copy = pltpu.make_async_remote_copy(
                src_ref=leaving.at[k],
                dst_ref=landed.at[k],
                send_sem=send.at[k],
                recv_sem=recv.at[k],
                device_id=block_at(place, sizes, -move),
                device_id_type=MESH,
            )
            copy.start()
            copies.append(copy)
        agg[...] = jnp.zeros_like(agg)

        def project(part, lo):
            span = pl.ds(lo, part.shape[0])
            proj_s[span, :] = product(part, win_ref[1]).astype(BF)
            proj_r[span, :] = product(part, win_ref[2]).astype(BF)

        project(mesh_ref[...], 0)
        project(coarse_ref[...], own + halo)
        for copy in copies:
            copy.wait()
        halo_ref[...] = landed[...].reshape(halo_ref.shape)
        project(halo_ref[...], own)

    send_col, recv_col, _, recv_row = edge_index(tiles_ref, own, halo)
    rows_in = lat_ref[...]
    pre = (
        product(rows_in, win_ref[0])
        + product(one_hot(send_col, (block, rows), 1), proj_s[...])
        + product(one_hot(recv_col, (block, rows), 1), proj_r[...])
    )
    sig = 1.0 / (1.0 + jnp.exp(-pre))
    hidden = (pre * sig).astype(BF)
    slope_ref[...] = (sig * (1.0 + pre * (1.0 - sig))).astype(BF)
    hid_ref[...] = hidden
    normed, inverse = normalize(product(hidden, wout_ref[...]))
    norm_ref[...] = normed.astype(BF)
    inv_ref[...] = inverse
    place = step * block + lax.broadcasted_iota(jnp.int32, (block, 1), 0)
    alive = jnp.where(place < live_ref[0] * tile_width, 1.0, 0.0)
    message = normed * gain_ref[...] * alive
    new_ref[...] = (rows_in.astype(F32) + message).astype(BF)
    agg[...] += product(one_hot(recv_row, (rows, block), 0), message.astype(BF))

    @pl.when(step == pl.num_programs(0) - 1)
    def _():
        agg_own[...] = agg[pl.ds(0, own), :].astype(BF)
        agg_coarse[...] = agg[pl.ds(own + halo, rows - own - halo), :].astype(BF)


def edge_backward(
    tile_width,
    factor,
    bits,
    sizes,
    moves,
    steps,
    node_cuts,
    edge_cuts,
    coarse_cuts,
    live_ref,
    lat_ref,
    grad_ref,
    hid_ref,
    slope_ref,
    norm_ref,
    inv_ref,
    tiles_ref,
    mesh_ref,
    halo_ref,
    coarse_ref,
    own_slope,
    coarse_slope,
    own_direct,
    direct_part,
    new_part,
    node_pack,
    node_gain,
    lists_ref,
    win_ref,
    wout_ref,
    gain_ref,
    edges_grad,
    edge_out,
    node_out,
    coarse_out,
    nodes_grad,
    edge_sum,
    node_sum,
    new_coarse,
    out_sems,
    coarse_sem,
    slots_table,
    sent,
    received,
    first_acc,
    out_acc,
    gain_acc,
    pre_all,
    pack,
    leaving,
    landed,
    send,
    recv,
    new_send,
    new_recv,
    *refs,
):
    step = pl.program_id(0)
    own, halo = mesh_ref.shape[0], halo_ref.shape[0]
    rows, d = slots_table.shape
    block = lat_ref.shape[0]
    coarse = coarse_ref.shape[0]
    place, count = here(), len(bits)
    kinds = sum_kinds(count)
    each = 2 * count + 3
    nodes = make_folds(place, bits, kinds, cut_parts(node_pack, node_sum, node_cuts), refs, d)
    refs = refs[each * len(nodes) :]
    groups, lo = [], 0
    for cuts in edge_cuts:
        group = []
        for size in cuts:
            group.append((pack, edge_sum, size, lo))
            lo += size
        groups.append(group)
    flat = make_folds(place, bits, kinds, [part for group in groups for part in group], refs, d)
    edges = []
    for group in groups:
        edges.append(flat[: len(group)])
        flat = flat[len(group) :]
    for number, fold in enumerate(nodes + [fold for group in edges for fold in group]):
        fold.out, fold.out_sem = (node_out if number < len(nodes) else edge_out), out_sems.at[number]
    shares = [
        Fold(place, turned(bits, number), coarse_kinds(count), None, target, lo, size, d, (), True)
        for number, (_, target, size, lo) in enumerate(cut_parts(None, new_coarse, coarse_cuts))
    ]
    wide = coarse_kinds(count).count("c")
    spans = [fold.region(fold.pending(fold.gather_order[wide]))[0] for fold in shares]

    def share_copy(number, turn):
        fold = shares[number]
        stage = fold.gather_order[turn]
        return fold.gather_copy(stage, new_coarse, (new_send.at[number], new_recv.at[number]))

    groups = {"n": nodes, "a": edges[0] + edges[1], "b": edges[4], "c": edges[2], "d": edges[3]}
    turns = {name: 0 for name in groups}

    def move(names):
        for name in names:
            if turns[name] < 2 * count:
                for fold in groups[name]:
                    fold.advance(turns[name])
                    if turns[name] == 2 * count - 1:
                        fold.deliver()
                turns[name] += 1
            if name == "n" and wide + turns["n"] <= count:
                for number in range(len(shares)):
                    share_copy(number, wide + turns["n"] - 1).wait()
                    if wide + turns["n"] < count:
                        share_copy(number, wide + turns["n"]).start()

    table = {0: "n", 2: "n", 3: "n", 5: "na", 7: "na", 8: "b", 9: "a", 10: "nb", 11: "a", 12: "nabcd", 13: "nabcd",
             14: "nabcd", 15: "nabcd"}

    @pl.when(step == 0)
    def _():
        greet([across(place, bit) for bit in bits] + [block_at(place, sizes, -move) for move in moves])
        for fold in nodes:
            fold.begin(0)
        at = 0
        for number, span in enumerate(spans):
            new_coarse[span, :] = new_part[pl.ds(at, span.size), :]
            at += span.size
            share_copy(number, wide).start()
        for acc in (sent, received, first_acc, out_acc, gain_acc):
            acc[...] = jnp.zeros_like(acc)
        slots_table[pl.ds(0, own), :] = own_slope[...]
        slots_table[pl.ds(own, halo), :] = jnp.zeros((halo, d), BF)
        slots_table[pl.ds(own + halo, coarse), :] = coarse_slope[...]

    @pl.when(step < steps)
    def _():
        _, recv_col, _, _ = edge_index(tiles_ref, own, halo)
        at_row = step * block + lax.broadcasted_iota(jnp.int32, (block, 1), 0)
        alive = jnp.where(at_row < live_ref[0] * tile_width, 1.0, 0.0)
        edge_slope = grad_ref[...].astype(F32)
        message_slope = (
            edge_slope + product(one_hot(recv_col, (block, rows), 1), slots_table[...])
        ) * alive
        normed = norm_ref[...].astype(F32)
        gain_acc[...] += jnp.sum(message_slope * normed, axis=0, keepdims=True)
        out_slope = normalize_back(message_slope * gain_ref[...], normed, inv_ref[...]).astype(BF)
        out_acc[...] += inner_rows(hid_ref[...], out_slope)
        pre_slope = (outer_cols(out_slope, wout_ref[...]) * slope_ref[...].astype(F32)).astype(BF)
        pre_all[pl.ds(pl.multiple_of(step * block, block), block), :] = pre_slope
        first_acc[...] += inner_rows(lat_ref[...], pre_slope)

    starts = [group[0].lo for group in edges]

    @pl.when(step == steps - 1)
    def _():
        pack[pl.ds(starts[0], d), :] = (first_acc[...] * factor).astype(BF)
        pack[pl.ds(starts[1], d), :] = (out_acc[...] * factor).astype(BF)
        for fold in groups["a"]:
            fold.begin(0)

    def scatter(kind, total):
        row = edge_index(tiles_ref, own, halo)[kind]
        at_block = pl.ds(pl.multiple_of(lax.rem(step, steps) * block, block), block)
        total[...] += product(one_hot(row, (rows, block), 0), pre_all[at_block, :])

    def weight_of(source):
        weight = None
        for part, lo in ((mesh_ref, 0), (halo_ref, own), (coarse_ref, own + halo)):
            term = inner_rows(part[...], source[pl.ds(lo, part.shape[0]), :].astype(BF))
            weight = term if weight is None else weight + term
        return (weight * factor).astype(BF)

    def back(lo, size):
        span = pl.ds(lo, size)
        return outer_cols(sent[span, :].astype(BF), win_ref[1]) + outer_cols(
            received[span, :].astype(BF), win_ref[2]
        )

    @pl.when(step // steps == 1)
    def _():
        scatter(3, received)

    @pl.when(step == 2 * steps - 1)
    def _():
        pack[pl.ds(starts[4], d), :] = weight_of(received)
        for fold in groups["b"]:
            fold.begin(0)

    @pl.when(step // steps == 2)
    def _():
        scatter(2, sent)

    slots = leaving.shape[1]

    def home_copy(k):
        return pltpu.make_async_remote_copy(
            src_ref=leaving.at[k],
            dst_ref=landed.at[k],
            send_sem=send.at[k],
            recv_sem=recv.at[k],
            device_id=block_at(place, sizes, moves[k]),
            device_id_type=MESH,
        )

    @pl.when(step == 3 * steps - 1)
    def _():
        pack[pl.ds(starts[2], coarse), :] = back(own + halo, coarse).astype(BF)
        at = 0
        for fold, span in zip(shares, spans):
            here_span = pl.ds(pl.multiple_of(starts[2] + span.start, 16), span.size)
            pack[here_span, :] = (
                pack[here_span, :].astype(F32) + direct_part[pl.ds(at, span.size), :]
            ).astype(BF)
            at += span.size
        rest = starts[3] - starts[2] - coarse
        which = lax.broadcasted_iota(jnp.int32, (rest, d), 0)
        pack[pl.ds(starts[2] + coarse, rest), :] = (
            jnp.where(which == 0, gain_acc[...], node_gain[...]) * factor
        ).astype(BF)
        for fold in groups["c"]:
            fold.begin(0)
        pack[pl.ds(starts[3], d), :] = weight_of(sent)
        for fold in groups["d"]:
            fold.begin(0)
        leave = back(own, halo).astype(BF)
        for k in range(len(moves)):
            leaving[k] = leave[k * slots : (k + 1) * slots]
        for k in range(len(moves)):
            home_copy(k).start()

    @pl.when(step // steps == 3)
    def _():
        at_block = pl.ds(pl.multiple_of((step - 3 * steps) * block, block), block)
        edges_grad[...] = (grad_ref[...].astype(F32) + outer_cols(pre_all[at_block, :], win_ref[0])).astype(BF)

    for part, names in table.items():

        @pl.when(step == part * 4 * steps // 16)
        def _():
            move(names)

    @pl.when(step == 4 * steps - 1)
    def _():
        direct = own_direct[...] + back(0, own)
        whole_coarse = pltpu.make_async_copy(new_coarse, coarse_out, coarse_sem)
        while wide + turns["n"] <= count:
            move("n")
        whole_coarse.start()
        while any(turn < 2 * count for turn in turns.values()):
            move("nabcd")
        for k in range(len(moves)):
            home_copy(k).wait()
        home = landed[...].reshape(halo, d)
        nodes_grad[...] = (direct + inner_rows(picks(lists_ref, own), home)).astype(BF)
        for name in groups:
            for fold in groups[name]:
                fold.delivery().wait()
        whole_coarse.wait()


def hand_out(
    starts,
    coarse,
    edge_sum,
    node_sum,
    new_coarse,
    nodes_grad,
    new_nodes,
    new_edges,
    edges_grad,
    edge_in,
    edge_out,
    coarse_grad,
    node_in,
    node_out,
    coarse_new,
    mesh_grad,
    mesh_new,
    edges_new,
    edges_back,
    edge_gain,
    node_gain,
    held,
    tail,
    come,
    leave,
    tail_sem,
):
    d = edge_sum.shape[1]
    last = pltpu.make_async_copy(edge_sum.at[pl.ds(starts[2] + coarse, tail.shape[0])], tail, tail_sem)
    last.start()
    jobs = hand_jobs(
        starts, coarse, edge_sum, node_sum, new_coarse, nodes_grad, new_nodes, new_edges, edges_grad, edge_in,
        edge_out, coarse_grad, node_in, node_out, coarse_new, mesh_grad, mesh_new, edges_new, edges_back,
    )
    moved, at = [], 0
    for number, (source, lo, target, target_lo, size) in enumerate(jobs):
        here_span = held.at[pl.ds(at, size)]
        at += size
        moved.append(
            (
                pltpu.make_async_copy(source.at[pl.ds(lo, size)], here_span, come.at[number]),
                pltpu.make_async_copy(here_span, target.at[pl.ds(target_lo, size)], leave.at[number]),
            )
        )
    for first, _ in moved:
        first.start()
    for first, second in moved:
        first.wait()
        second.start()
    last.wait()
    edge_gain[...] = tail[pl.ds(0, 1), :].astype(F32)
    node_gain[...] = tail[pl.ds(1, 1), :].astype(F32)
    for _, second in moved:
        second.wait()


def hand_jobs(
    starts, coarse, edge_sum, node_sum, new_coarse, nodes_grad, new_nodes, new_edges, edges_grad, edge_in,
    edge_out, coarse_grad, node_in, node_out, coarse_new, mesh_grad, mesh_new, edges_new, edges_back,
):
    d, own, edges = edge_sum.shape[1], new_nodes.shape[0], new_edges.shape[0]
    jobs = []
    for source, target in ((new_edges, edges_new), (edges_grad, edges_back)):
        jobs += [(source, lo, target, lo, d) for lo in range(0, edges, d)]
    jobs += [(node_sum, 0, node_in, 0, d), (node_sum, d, node_in, d, d), (node_sum, 2 * d, node_out, 0, d)]
    jobs += [(new_coarse, 0, coarse_new, 0, coarse), (new_nodes, 0, mesh_new, 0, own)]
    jobs += [(edge_sum, starts[0], edge_in, 0, d), (edge_sum, starts[3], edge_in, d, d)]
    jobs += [(edge_sum, starts[4], edge_in, 2 * d, d), (edge_sum, starts[1], edge_out, 0, d)]
    return jobs + [(edge_sum, starts[2], coarse_grad, 0, coarse), (nodes_grad, 0, mesh_grad, 0, own)]


def whole(shape):
    zero = (0,) * len(shape)
    return pl.BlockSpec(shape, lambda i: zero)


def by_rows(block, width):
    return pl.BlockSpec((block, width), lambda i: (i, 0))


def by_cols(block):
    return pl.BlockSpec((1, block), lambda i: (0, i))


def shape_of(shape, dtype):
    return jax.ShapeDtypeStruct(shape, dtype)


def cost(flops, moved):
    return pl.CostEstimate(flops=int(flops), bytes_accessed=int(moved), transcendentals=0)


PARAMS = dict(
    compiler_params=pltpu.CompilerParams(
        dimension_semantics=("arbitrary",), vmem_limit_bytes=60 * 1024 * 1024
    )
)


def talking(number, grid=False):
    return pltpu.CompilerParams(
        collective_id=number,
        has_side_effects=True,
        vmem_limit_bytes=60 * 1024 * 1024,
        dimension_semantics=("arbitrary",) if grid else None,
    )


def on_device(
    mesh_nodes,
    coarse_nodes,
    edge_latents,
    edge_tiles,
    send_lists,
    tiles_live,
    edge_in,
    edge_out,
    edge_gain,
    node_in,
    node_out,
    node_gain,
    grad_nodes,
    grad_coarse,
    grad_edges,
):
    sizes = tuple(lax.axis_size(axis) for axis in AXES)
    block_count = sizes[0] * sizes[1]
    bits = square_bits(sizes)
    count = len(bits)
    own, d = mesh_nodes.shape
    neigh, slots = send_lists.shape[1:]
    coarse = coarse_nodes.shape[0]
    halo = neigh * slots
    rows = own + halo + coarse
    tile_dev, _, tile_width = edge_tiles.shape
    edges = tile_dev * tile_width
    tiles = 4 if tile_dev % 4 == 0 else 1
    block = tiles * tile_width
    moves = cycle_moves(neigh, block_count)
    factor = float(edges * block_count) ** (-0.5)
    e_gain, n_gain = edge_gain.reshape(1, d), node_gain.reshape(1, d)
    vmem = pl.BlockSpec(memory_space=pltpu.VMEM)
    smem = pl.BlockSpec(memory_space=pltpu.SMEM)
    wide, col = by_rows(block, d), by_rows(block, 1)
    pairs = pl.BlockSpec((tiles, 2, tile_width), lambda i: (i, 0, 0))
    tables = [whole((own, d)), whole((halo, d)), whole((coarse, d))]
    weights = [whole((3, d, d)), whole((d, d)), whole((1, d))]
    swap = [pltpu.VMEM((neigh, slots, d), BF)] * 2 + [pltpu.SemaphoreType.DMA((neigh,))] * 2
    new_edges, hidden, slope, normed, inverse, agg_own, agg_coarse, incoming = pl.pallas_call(
        functools.partial(edge_forward, tile_width, sizes, moves),
        grid=(edges // block,),
        in_specs=[smem, wide, pairs, whole((1, neigh, slots)), tables[0], tables[2]] + weights,
        out_specs=[wide] * 4 + [col, tables[0], tables[2], tables[1]],
        out_shape=[shape_of((edges, d), BF)] * 4
        + [
            shape_of((edges, 1), F32),
            shape_of((own, d), BF),
            shape_of((coarse, d), BF),
            shape_of((halo, d), BF),
        ],
        scratch_shapes=[
            pltpu.VMEM((rows, d), BF),
            pltpu.VMEM((rows, d), BF),
            pltpu.VMEM((rows, d), F32),
        ]
        + swap,
        cost_estimate=cost(2 * edges * d * (3 * rows + 2 * d), 12 * edges * d),
        compiler_params=talking(0, grid=True),
    )(
        tiles_live, edge_latents, edge_tiles, send_lists, mesh_nodes, coarse_nodes, edge_in, edge_out, e_gain
    )
    sum_rows = padded(coarse, count)
    grown = [agg_coarse, coarse_nodes, grad_coarse]
    if sum_rows > coarse:
        grown = [jnp.pad(array, ((0, sum_rows - coarse), (0, 0))) for array in grown]
    coarse_rows = split_rows(sum_rows, count, 3)
    share_rows = sum_rows // 2 ** (count - 2)
    all_rows = own + share_rows
    node_rows = padded(3 * d, count)
    parts = len(coarse_rows)
    new_nodes, new_part, own_slope, c_slope, own_direct, direct_part, node_pack, node_gain_part = pl.pallas_call(
        functools.partial(middle_step, bits, coarse_rows, factor),
        in_specs=[vmem] * 9,
        out_specs=[vmem] * 8,
        out_shape=[
            shape_of((own, d), BF),
            shape_of((share_rows, d), BF),
            shape_of((own, d), BF),
            shape_of((sum_rows, d), BF),
            shape_of((own, d), F32),
            shape_of((share_rows, d), F32),
            shape_of((node_rows, d), BF),
            shape_of((1, d), F32),
        ],
        scratch_shapes=[pltpu.VMEM((sum_rows, d), BF)]
        + [pltpu.VMEM((all_rows, d), BF)] * 5
        + [pltpu.SemaphoreType.DMA((parts, count))] * 2
        + fold_scratch(coarse_kinds(count), coarse_rows, d),
        compiler_params=talking(1),
    )(agg_own, grown[0], mesh_nodes, grown[1], grad_nodes, grown[2], node_in, node_out, n_gain)
    if sum_rows > coarse:
        c_slope = c_slope[:coarse]
    sections = [d, d, coarse + 2, d, d]
    edge_cuts = [split_rows(section, count, 2) for section in sections]
    node_cuts = split_rows(node_rows, count, 3)
    starts = [sum(sum(cuts) for cuts in edge_cuts[:i]) for i in range(len(sections))]
    edge_rows = sum(sum(cuts) for cuts in edge_cuts)
    steps = edges // block

    away = pl.BlockSpec(memory_space=pl.ANY)
    cuts = node_cuts + [size for section in edge_cuts for size in section]

    def once(width):
        return pl.BlockSpec((block, width), lambda i: (i - ((i // steps + 3) // 4) * (i - (steps - 1)), 0))

    again = pl.BlockSpec((block, d), lambda i: (lax.rem(i, steps), 0))
    again_pairs = pl.BlockSpec((tiles, 2, tile_width), lambda i: (lax.rem(i, steps), 0, 0))
    later = pl.BlockSpec((block, d), lambda i: ((i // (3 * steps)) * (i - 3 * steps), 0))
    edges_grad, edge_sum, node_sum, new_coarse, nodes_grad = pl.pallas_call(
        functools.partial(
            edge_backward, tile_width, factor, bits, sizes, moves, steps, node_cuts, edge_cuts, coarse_rows
        ),
        grid=(4 * steps,),
        in_specs=[smem, once(d), again] + [once(d)] * 3 + [once(1), again_pairs] + [vmem] * 14,
        out_specs=[later] + [away] * 3 + [vmem],
        out_shape=[
            shape_of((edges, d), BF),
            shape_of((edge_rows, d), BF),
            shape_of((node_rows, d), BF),
            shape_of((sum_rows, d), BF),
            shape_of((own, d), BF),
        ],
        scratch_shapes=[
            pltpu.VMEM((edge_rows, d), BF),
            pltpu.VMEM((node_rows, d), BF),
            pltpu.VMEM((sum_rows, d), BF),
            pltpu.SemaphoreType.DMA((len(cuts),)),
            pltpu.SemaphoreType.DMA,
            pltpu.VMEM((rows, d), BF),
            pltpu.VMEM((rows, d), F32),
            pltpu.VMEM((rows, d), F32),
            pltpu.VMEM((d, d), F32),
            pltpu.VMEM((d, d), F32),
            pltpu.VMEM((1, d), F32),
            pltpu.VMEM((edges, d), BF),
            pltpu.VMEM((edge_rows, d), BF),
        ]
        + swap
        + [pltpu.SemaphoreType.DMA((parts, count))] * 2
        + fold_scratch(sum_kinds(count), cuts, d),
        cost_estimate=cost(2 * edges * d * (3 * rows + 4 * d), 14 * edges * d),
        compiler_params=talking(2, grid=True),
    )(
        tiles_live, edge_latents, grad_edges, hidden, slope, normed, inverse, edge_tiles, mesh_nodes, incoming,
        coarse_nodes, own_slope, c_slope, own_direct, direct_part, new_part, node_pack, node_gain_part, send_lists,
        edge_in, edge_out, e_gain,
    )
    sources = [edge_sum, node_sum, new_coarse, nodes_grad, new_nodes, new_edges, edges_grad]
    results = [
        shape_of((3 * d, d), BF),
        shape_of((d, d), BF),
        shape_of((coarse, d), BF),
        shape_of((2 * d, d), BF),
        shape_of((d, d), BF),
        shape_of((coarse, d), BF),
        shape_of((own, d), BF),
        shape_of((own, d), BF),
        shape_of((edges, d), BF),
        shape_of((edges, d), BF),
    ]
    jobs = hand_jobs(starts, coarse, *sources, *results)
    (
        g_in,
        g_out,
        coarse_grad,
        n_in,
        n_out,
        coarse_new,
        mesh_grad,
        mesh_new,
        new_edges,
        edges_grad,
        edge_gain_grad,
        node_gain_grad,
    ) = pl.pallas_call(
        functools.partial(hand_out, starts, coarse),
        in_specs=[away] * len(sources),
        out_specs=[away] * len(results) + [vmem] * 2,
        out_shape=results + [shape_of((1, d), F32)] * 2,
        scratch_shapes=[
            pltpu.VMEM((sum(job[-1] for job in jobs), d), BF),
            pltpu.VMEM((16, d), BF),
            pltpu.SemaphoreType.DMA((len(jobs),)),
            pltpu.SemaphoreType.DMA((len(jobs),)),
            pltpu.SemaphoreType.DMA,
        ],
        compiler_params=pltpu.CompilerParams(vmem_limit_bytes=60 * 1024 * 1024),
    )(*sources)
    return (
        mesh_new,
        coarse_new,
        new_edges,
        mesh_grad,
        coarse_grad,
        edges_grad,
        g_in.reshape(3, d, d),
        g_out,
        edge_gain_grad[0],
        n_in.reshape(2, d, d),
        n_out,
        node_gain_grad[0],
    )


def solution(mesh):
    rows2 = P(AXES, None)
    rows3 = P(AXES, None, None)
    in_specs = (
        rows2, P(), rows2, rows3, rows3, P(AXES), P(), P(), P(), P(), P(), P(), rows2, P(), rows2,
    )
    out_specs = (rows2, P(), rows2, rows2, P(), rows2, P(), P(), P(), P(), P(), P())
    return jax.shard_map(
        on_device, mesh=mesh, in_specs=in_specs, out_specs=out_specs, check_vma=False
    )
```

```python
import functools

import jax
import jax.numpy as jnp
from jax import lax
from jax.experimental import pallas as pl
from jax.experimental.pallas import tpu as pltpu
from jax.sharding import PartitionSpec as P

EPS = 1e-05
BF = jnp.bfloat16
F32 = jnp.float32
AXES = ("lat", "blk")
MESH = pl.DeviceIdType.MESH


def dims(a, b, ca, cb):
    return lax.dot_general(a, b, (((ca,), (cb,)), ((), ())), preferred_element_type=F32)


def product(a, b):
    return dims(a, b, 1, 0)


def inner_rows(a, b):
    return dims(a, b, 0, 0)


def outer_cols(a, b):
    return dims(a, b, 1, 1)


def normalize(values):
    centered = values - jnp.mean(values, axis=-1, keepdims=True)
    inverse = lax.rsqrt(jnp.mean(centered * centered, axis=-1, keepdims=True) + EPS)
    return (centered * inverse, inverse)


def normalize_back(upstream, normed, inverse):
    return inverse * (
        upstream
        - jnp.mean(upstream, axis=-1, keepdims=True)
        - normed * jnp.mean(upstream * normed, axis=-1, keepdims=True)
    )


def one_hot(index, shape, axis):
    return jnp.where(lax.broadcasted_iota(jnp.int32, shape, axis) == index, 1.0, 0.0).astype(BF)


def cycle_moves(neigh_count, block_count):
    near_count = neigh_count // 2 - 1
    near = [position - near_count for position in range(near_count)] + [
        position + 1 for position in range(near_count)
    ]
    return near + [block_count // 4, block_count // 2]


def square_bits(sizes):
    found = []
    for axis, size in zip(AXES, sizes):
        step = 1
        while step < size:
            found.append((axis, step))
            step *= 2
        assert step == size
    return found


def turned(bits, turn):
    middle = bits[1:-1]
    turn = turn % len(middle)
    return [bits[0]] + middle[turn:] + middle[:turn] + [bits[-1]]


def bit_of(place, bit):
    return lax.rem(place[bit[0]] // bit[1], 2)


def across(place, bit):
    axis, step = bit
    moved = dict(place)
    moved[axis] = place[axis] + step - 2 * step * bit_of(place, bit)
    return tuple(moved[axis] for axis in AXES)


def here():
    return {axis: lax.axis_index(axis) for axis in AXES}


class Fold:
    def __init__(self, place, order, kinds, source, target, lo, rows, cols, refs, wide_first=False):
        count = len(order)
        self.place, self.order, self.kinds = place, order, kinds
        self.source, self.target, self.lo = source, target, lo
        self.rows, self.cols = rows, cols
        self.arrive, self.held = refs[:count], refs[count : 2 * count - 1]
        if refs:
            self.rs_send, self.rs_recv, self.ag_send, self.ag_recv = refs[2 * count - 1 :]
        self.sizes = Fold.shapes(kinds, rows, cols)
        self.gather_order = list(reversed(range(count)))
        if wide_first:
            self.gather_order.sort(key=lambda stage: kinds[stage] == "r")

    @staticmethod
    def shapes(kinds, rows, cols):
        found = []
        for kind in kinds:
            if kind == "c":
                cols //= 2
            else:
                rows //= 2
            found.append((rows, cols))
        return found

    @staticmethod
    def scratch(kinds, rows, cols):
        shapes, count = Fold.shapes(kinds, rows, cols), len(kinds)
        return (
            [pltpu.VMEM(shape, BF) for shape in shapes]
            + [pltpu.VMEM(shape, BF) for shape in shapes[:-1]]
            + [pltpu.SemaphoreType.DMA((count,))] * 4
        )

    def halves(self, stage):
        rows, cols = self.sizes[stage]
        bit = bit_of(self.place, self.order[stage])
        if self.kinds[stage] == "c":
            mine, other = pl.multiple_of(bit * cols, 128), pl.multiple_of((1 - bit) * cols, 128)
            return rows, (0, pl.ds(mine, cols)), (0, pl.ds(other, cols))
        mine, other = pl.multiple_of(bit * rows, 16), pl.multiple_of((1 - bit) * rows, 16)
        return rows, (mine, pl.ds(0, cols)), (other, pl.ds(0, cols))

    def previous(self, stage):
        return (self.source, self.lo) if stage == 0 else (self.held[stage - 1], 0)

    def reduce_copy(self, stage):
        rows, _, (start, span) = self.halves(stage)
        ref, base = self.previous(stage)
        return pltpu.make_async_remote_copy(
            src_ref=ref.at[pl.ds(base + start, rows), span],
            dst_ref=self.arrive[stage],
            send_sem=self.rs_send.at[stage],
            recv_sem=self.rs_recv.at[stage],
            device_id=across(self.place, self.order[stage]),
            device_id_type=MESH,
        )

    def region(self, pending):
        row, col, rows, cols = self.lo, 0, self.rows, self.cols
        for stage in pending:
            bit = bit_of(self.place, self.order[stage])
            if self.kinds[stage] == "c":
                cols //= 2
                col = col + bit * cols
            else:
                rows //= 2
                row = row + bit * rows
        return pl.ds(pl.multiple_of(row, 16), rows), pl.ds(pl.multiple_of(col, 128), cols)

    def pending(self, stage):
        return sorted(self.gather_order[self.gather_order.index(stage) :])

    def add(self, stage):
        rows, (start, span), _ = self.halves(stage)
        ref, base = self.previous(stage)
        last = stage == len(self.order) - 1
        piece = next(size for size in (128, 96, 80, 64, 48, 32, 16) if rows % size == 0)
        if last:
            row_at, col_at = self.region(range(len(self.order)))

        def one(step, carry):
            at = pl.multiple_of(step * piece, 16)
            total = ref[pl.ds(base + start + at, piece), span].astype(F32) + self.arrive[stage][
                pl.ds(at, piece), :
            ].astype(F32)
            if last:
                self.target[pl.ds(pl.multiple_of(row_at.start + at, 16), piece), col_at] = total.astype(BF)
            else:
                self.held[stage][pl.ds(at, piece), :] = total.astype(BF)
            return carry

        if rows == piece:
            one(0, 0)
        else:
            lax.fori_loop(0, rows // piece, one, 0)

    def gather_copy(self, stage, target=None, sems=None):
        span = (self.target if target is None else target).at[self.region(self.pending(stage))]
        send, recv = (self.ag_send, self.ag_recv) if sems is None else sems
        return pltpu.make_async_remote_copy(
            src_ref=span,
            dst_ref=span,
            send_sem=send.at[stage],
            recv_sem=recv.at[stage],
            device_id=across(self.place, self.order[stage]),
            device_id_type=MESH,
        )


    def delivery(self):
        span = pl.ds(self.lo, self.rows)
        return pltpu.make_async_copy(self.target.at[span, :], self.out.at[span, :], self.out_sem)

    def deliver(self):
        self.delivery().start()

    def begin(self, turn):
        count = len(self.order)
        if turn < count:
            self.reduce_copy(turn).start()
        elif turn < 2 * count:
            self.gather_copy(self.gather_order[turn - count]).start()

    def advance(self, turn):
        count = len(self.order)
        if turn < count:
            self.reduce_copy(turn).wait_recv()
            self.add(turn)
        else:
            self.gather_copy(self.gather_order[turn - count]).wait_recv()
        self.begin(turn + 1)

    def drain(self):
        for stage in range(len(self.order)):
            self.reduce_copy(stage).wait_send()
            self.gather_copy(stage).wait_send()


def sum_kinds(count):
    return ["c", "c"] + ["r"] * (count - 2)


def coarse_kinds(count):
    return ["r", "c", "c"] + ["r"] * (count - 3)


def fold_scratch(kinds, rows, cols):
    scratch = []
    for part in rows:
        scratch += Fold.scratch(kinds, part, cols)
    return scratch


def make_folds(place, bits, kinds, parts, refs, cols, wide_first=False):
    count, folds = len(bits), []
    for number, (source, target, rows, lo) in enumerate(parts):
        mine, refs = refs[: 2 * count + 3], refs[2 * count + 3 :]
        order = turned(bits, number)
        folds.append(Fold(place, order, kinds, source, target, lo, rows, cols, mine, wide_first))
    return folds


def cut_parts(source, target, sizes):
    parts, lo = [], 0
    for rows in sizes:
        parts.append((source, target, rows, lo))
        lo += rows
    return parts


def greet(devices):
    barrier = pltpu.get_barrier_semaphore()
    for device in devices:
        pl.semaphore_signal(barrier, inc=1, device_id=device, device_id_type=MESH)
    pl.semaphore_wait(barrier, len(devices))


def split_rows(rows, count, pieces):
    unit = 16 * 2 ** (count - 2)
    units = -(-rows // unit)
    pieces = min(pieces, units)
    sizes = [unit * (units // pieces + (1 if i < units % pieces else 0)) for i in range(pieces)]
    return sizes


def padded(rows, count):
    return sum(split_rows(rows, count, 1))


def block_at(place, sizes, move):
    total = sizes[0] * sizes[1]
    block = lax.rem(place[AXES[0]] * sizes[1] + place[AXES[1]] + (move % total), total)
    return block // sizes[1], lax.rem(block, sizes[1])


def picks(lists_ref, own):
    _, neigh, slots = lists_ref.shape
    listed = lists_ref[0].T
    return jnp.concatenate(
        [one_hot(listed[:, k : k + 1], (slots, own), 1).astype(F32) for k in range(neigh)], axis=0
    ).astype(BF)


def node_math(rows, summed, slope, win_ref, wout_ref, gain):
    pre = product(rows, win_ref[0]) + product(summed, win_ref[1])
    sig = 1.0 / (1.0 + jnp.exp(-pre))
    hidden = (pre * sig).astype(BF)
    normed, inverse = normalize(product(hidden, wout_ref[...]))
    new = (rows.astype(F32) + normed * gain).astype(BF)
    out_slope = normalize_back(slope * gain, normed, inverse).astype(BF)
    swish = sig * (1.0 + pre * (1.0 - sig))
    pre_slope = (outer_cols(out_slope, wout_ref[...]) * swish).astype(BF)
    back = outer_cols(pre_slope, win_ref[1]).astype(BF)
    direct = slope + outer_cols(pre_slope, win_ref[0])
    return new, back, direct, slope * normed, hidden, out_slope, pre_slope


def middle_step(
    bits,
    part_rows,
    factor,
    own_sum,
    coarse_part,
    mesh_ref,
    coarse_ref,
    grad_ref,
    grad_coarse,
    win_ref,
    wout_ref,
    gain_ref,
    new_nodes,
    new_part,
    own_slope,
    coarse_slope,
    own_direct,
    direct_part,
    pack,
    node_gain,
    total,
    all_rows,
    all_sums,
    all_hidden,
    all_out,
    all_pre,
    slope_send,
    slope_recv,
    *refs,
):
    place = here()
    greet([across(place, bit) for bit in bits])
    count, kinds = len(bits), coarse_kinds(len(bits))
    own, d = mesh_ref.shape
    coarse = coarse_ref.shape[0]
    folds = make_folds(place, bits, kinds, cut_parts(coarse_part, total, part_rows), refs, d, True)
    for fold in folds:
        fold.reduce_copy(0).start()
    gain = gain_ref[...]
    gains = [jnp.zeros((1, d), F32)]
    pieces = 4 if own % 64 == 0 else 1
    piece = own // pieces

    def own_piece(number):
        span = pl.ds(number * piece, piece)
        results = node_math(
            mesh_ref[span, :], own_sum[span, :], grad_ref[span, :].astype(F32), win_ref, wout_ref, gain
        )
        new_nodes[span, :], own_slope[span, :], own_direct[span, :] = results[:3]
        gains.append(jnp.sum(results[3], axis=0, keepdims=True))
        all_rows[span, :], all_sums[span, :] = mesh_ref[span, :], own_sum[span, :]
        all_hidden[span, :], all_out[span, :], all_pre[span, :] = results[4:]

    todo = list(range(pieces))
    for stage in range(count):
        if todo:
            own_piece(todo.pop(0))
        for fold in folds:
            fold.reduce_copy(stage).wait_recv()
            fold.add(stage)
            if stage + 1 < count:
                fold.reduce_copy(stage + 1).start()
            else:
                fold.gather_copy(fold.gather_order[0]).start()
    while todo:
        own_piece(todo.pop(0))
    wide = kinds.count("c")
    for turn in range(wide):
        for fold in folds:
            fold.gather_copy(fold.gather_order[turn]).wait_recv()
            if turn + 1 < wide:
                fold.gather_copy(fold.gather_order[turn + 1]).start()
    spans, shares = [], []
    for fold in folds:
        span, _ = fold.region(fold.pending(fold.gather_order[wide]))
        first = 1
        for stage in range(count):
            if kinds[stage] == "c":
                first = first * (1 - bit_of(place, fold.order[stage]))
        spans.append(span)
        shares.append(jnp.full((span.size, 1), first, jnp.int32).astype(F32))
    share = jnp.concatenate(shares, axis=0)
    rows = jnp.concatenate([coarse_ref[span, :] for span in spans], axis=0)
    summed = jnp.concatenate([total[span, :] for span in spans], axis=0)
    slope = jnp.concatenate([grad_coarse[span, :] for span in spans], axis=0).astype(F32)
    new, back, direct, gain_term, hidden, out_slope, pre_slope = node_math(
        rows, summed, slope, win_ref, wout_ref, gain
    )
    new_part[...] = new
    direct_part[...] = direct * share
    at = 0
    for fold, span in zip(folds, spans):
        coarse_slope[span, :] = back[at : at + span.size]
        at += span.size
    tail = range(wide, count)

    def tail_copy(number, fold, turn):
        stage = fold.gather_order[turn]
        return fold.gather_copy(stage, coarse_slope, (slope_send.at[number], slope_recv.at[number]))

    for number, fold in enumerate(folds):
        tail_copy(number, fold, wide).start()
    span = pl.ds(own, at)
    all_rows[span, :], all_sums[span, :] = rows, summed
    all_hidden[span, :] = (hidden.astype(F32) * share).astype(BF)
    all_out[span, :] = out_slope
    all_pre[span, :] = (pre_slope.astype(F32) * share).astype(BF)
    gains.append(jnp.sum(gain_term * share, axis=0, keepdims=True))
    jobs = [
        lambda: (0, inner_rows(all_rows[...], all_pre[...])),
        lambda: (d, inner_rows(all_sums[...], all_pre[...])),
        lambda: (2 * d, inner_rows(all_hidden[...], all_out[...])),
    ]
    for turn in tail:
        if jobs:
            lo, result = jobs.pop(0)()
            pack[pl.ds(lo, d), :] = (result * factor).astype(BF)
        for number, fold in enumerate(folds):
            tail_copy(number, fold, turn).wait_recv()
            if turn + 1 < count:
                tail_copy(number, fold, turn + 1).start()
    assert not jobs
    for number, fold in enumerate(folds):
        for stage in range(count):
            fold.reduce_copy(stage).wait_send()
        for turn in range(wide):
            fold.gather_copy(fold.gather_order[turn]).wait_send()
        for turn in tail:
            tail_copy(number, fold, turn).wait_send()
    node_gain[...] = sum(gains)


def edge_index(tiles_ref, own, halo):
    count, _, width = tiles_ref.shape
    flat = tiles_ref[...].reshape(2 * count, width)
    fine = jnp.where(flat < own, flat, flat + halo)
    row = lax.broadcasted_iota(jnp.int32, flat.shape, 0)
    flat = jnp.where(lax.rem(row, 2) == 0, flat, fine)
    turned_flat = flat.T
    send_col = jnp.concatenate([turned_flat[:, 2 * t : 2 * t + 1] for t in range(count)], axis=0)
    recv_col = jnp.concatenate([turned_flat[:, 2 * t + 1 : 2 * t + 2] for t in range(count)], axis=0)
    send_row = jnp.concatenate([flat[2 * t : 2 * t + 1, :] for t in range(count)], axis=1)
    recv_row = jnp.concatenate([flat[2 * t + 1 : 2 * t + 2, :] for t in range(count)], axis=1)
    return send_col, recv_col, send_row, recv_row


def edge_forward(
    tile_width,
    sizes,
    moves,
    live_ref,
    lat_ref,
    tiles_ref,
    lists_ref,
    mesh_ref,
    coarse_ref,
    win_ref,
    wout_ref,
    gain_ref,
    new_ref,
    hid_ref,
    slope_ref,
    norm_ref,
    inv_ref,
    agg_own,
    agg_coarse,
    halo_ref,
    proj_s,
    proj_r,
    agg,
    sums_ref,
    leaving,
    landed,
    send,
    recv,
):
    step = pl.program_id(0)
    own, halo = mesh_ref.shape[0], halo_ref.shape[0]
    rows = agg.shape[0]
    block = lat_ref.shape[0]

    @pl.when(step == 0)
    def _():
        place = here()
        greet([block_at(place, sizes, move) for move in moves])
        slots = leaving.shape[1]
        rows_out = product(picks(lists_ref, own), mesh_ref[...]).astype(BF)
        copies = []
        for k, move in enumerate(moves):
            leaving[k] = rows_out[k * slots : (k + 1) * slots]
        for k, move in enumerate(moves):
            copy = pltpu.make_async_remote_copy(
                src_ref=leaving.at[k],
                dst_ref=landed.at[k],
                send_sem=send.at[k],
                recv_sem=recv.at[k],
                device_id=block_at(place, sizes, -move),
                device_id_type=MESH,
            )
            copy.start()
            copies.append(copy)
        agg[...] = jnp.zeros_like(agg)

        def project(part, lo):
            span = pl.ds(lo, part.shape[0])
            proj_s[span, :] = product(part, win_ref[1]).astype(BF)
            proj_r[span, :] = product(part, win_ref[2]).astype(BF)

        project(mesh_ref[...], 0)
        project(coarse_ref[...], own + halo)
        for copy in copies:
            copy.wait()
        halo_ref[...] = landed[...].reshape(halo_ref.shape)
        project(halo_ref[...], own)

    send_col, recv_col, _, recv_row = edge_index(tiles_ref, own, halo)
    halves = 2 if block % 256 == 0 else 1
    half = block // halves
    for part in range(halves):
        span = pl.ds(part * half, half)
        at = slice(part * half, (part + 1) * half)
        rows_in = lat_ref[span, :]
        pre = (
            product(rows_in, win_ref[0])
            + product(one_hot(send_col[at], (half, rows), 1), proj_s[...])
            + product(one_hot(recv_col[at], (half, rows), 1), proj_r[...])
        )
        sig = 1.0 / (1.0 + jnp.exp(-pre))
        hidden = (pre * sig).astype(BF)
        slope_ref[span, :] = (sig * (1.0 + pre * (1.0 - sig))).astype(BF)
        hid_ref[span, :] = hidden
        normed, inverse = normalize(product(hidden, wout_ref[...]))
        norm_ref[span, :] = normed.astype(BF)
        inv_ref[span, :] = inverse
        place = step * block + part * half + lax.broadcasted_iota(jnp.int32, (half, 1), 0)
        alive = jnp.where(place < live_ref[0] * tile_width, 1.0, 0.0)
        message = normed * gain_ref[...] * alive
        new_ref[span, :] = (rows_in.astype(F32) + message).astype(BF)
        sums_ref[span, :] = message.astype(BF)
    agg[...] += product(one_hot(recv_row, (rows, block), 0), sums_ref[...])

    @pl.when(step == pl.num_programs(0) - 1)
    def _():
        agg_own[...] = agg[pl.ds(0, own), :].astype(BF)
        agg_coarse[...] = agg[pl.ds(own + halo, rows - own - halo), :].astype(BF)


def edge_backward(
    tile_width,
    factor,
    bits,
    sizes,
    moves,
    steps,
    node_cuts,
    edge_cuts,
    coarse_cuts,
    live_ref,
    lat_ref,
    grad_ref,
    hid_ref,
    slope_ref,
    norm_ref,
    inv_ref,
    tiles_ref,
    mesh_ref,
    halo_ref,
    coarse_ref,
    own_slope,
    coarse_slope,
    own_direct,
    direct_part,
    new_part,
    node_pack,
    node_gain,
    lists_ref,
    win_ref,
    wout_ref,
    gain_ref,
    edges_grad,
    edge_out,
    node_out,
    coarse_out,
    nodes_grad,
    edge_sum,
    node_sum,
    new_coarse,
    out_sems,
    coarse_sem,
    slots_table,
    sent,
    received,
    first_acc,
    out_acc,
    gain_acc,
    pre_all,
    pack,
    leaving,
    landed,
    send,
    recv,
    new_send,
    new_recv,
    *refs,
):
    step = pl.program_id(0)
    own, halo = mesh_ref.shape[0], halo_ref.shape[0]
    rows, d = slots_table.shape
    block = lat_ref.shape[0]
    coarse = coarse_ref.shape[0]
    place, count = here(), len(bits)
    kinds = sum_kinds(count)
    each = 2 * count + 3
    nodes = make_folds(place, bits, kinds, cut_parts(node_pack, node_sum, node_cuts), refs, d)
    refs = refs[each * len(nodes) :]
    groups, lo = [], 0
    for cuts in edge_cuts:
        group = []
        for size in cuts:
            group.append((pack, edge_sum, size, lo))
            lo += size
        groups.append(group)
    flat = make_folds(place, bits, kinds, [part for group in groups for part in group], refs, d)
    edges = []
    for group in groups:
        edges.append(flat[: len(group)])
        flat = flat[len(group) :]
    for number, fold in enumerate(nodes + [fold for group in edges for fold in group]):
        fold.out, fold.out_sem = (node_out if number < len(nodes) else edge_out), out_sems.at[number]
    shares = [
        Fold(place, turned(bits, number), coarse_kinds(count), None, target, lo, size, d, (), True)
        for number, (_, target, size, lo) in enumerate(cut_parts(None, new_coarse, coarse_cuts))
    ]
    wide = coarse_kinds(count).count("c")
    spans = [fold.region(fold.pending(fold.gather_order[wide]))[0] for fold in shares]

    def share_copy(number, turn):
        fold = shares[number]
        stage = fold.gather_order[turn]
        return fold.gather_copy(stage, new_coarse, (new_send.at[number], new_recv.at[number]))

    groups = {"n": nodes, "a": edges[0] + edges[1], "b": edges[4], "c": edges[2], "d": edges[3]}
    turns = {name: 0 for name in groups}

    def move(names):
        for name in names:
            if turns[name] < 2 * count:
                for fold in groups[name]:
                    fold.advance(turns[name])
                    if turns[name] == 2 * count - 1:
                        fold.deliver()
                turns[name] += 1
            if name == "n" and wide + turns["n"] <= count:
                for number in range(len(shares)):
                    share_copy(number, wide + turns["n"] - 1).wait()
                    if wide + turns["n"] < count:
                        share_copy(number, wide + turns["n"]).start()

    table = {0: "n", 3: "n", 6: "n", 7: "a", 9: "n", 10: "b", 11: "a", 12: "cdnab", 13: "cdnab",
             14: "cdnab", 15: "cdnab"}

    @pl.when(step == 0)
    def _():
        greet([across(place, bit) for bit in bits] + [block_at(place, sizes, -move) for move in moves])
        for fold in nodes:
            fold.begin(0)
        at = 0
        for number, span in enumerate(spans):
            new_coarse[span, :] = new_part[pl.ds(at, span.size), :]
            at += span.size
            share_copy(number, wide).start()
        for acc in (sent, received, first_acc, out_acc, gain_acc):
            acc[...] = jnp.zeros_like(acc)
        slots_table[pl.ds(0, own), :] = own_slope[...]
        slots_table[pl.ds(own, halo), :] = jnp.zeros((halo, d), BF)
        slots_table[pl.ds(own + halo, coarse), :] = coarse_slope[...]

    @pl.when(step < steps)
    def _():
        _, recv_col, _, _ = edge_index(tiles_ref, own, halo)
        at_row = step * block + lax.broadcasted_iota(jnp.int32, (block, 1), 0)
        alive = jnp.where(at_row < live_ref[0] * tile_width, 1.0, 0.0)
        edge_slope = grad_ref[...].astype(F32)
        message_slope = (
            edge_slope + product(one_hot(recv_col, (block, rows), 1), slots_table[...])
        ) * alive
        normed = norm_ref[...].astype(F32)
        gain_acc[...] += jnp.sum(message_slope * normed, axis=0, keepdims=True)
        out_slope = normalize_back(message_slope * gain_ref[...], normed, inv_ref[...]).astype(BF)
        out_acc[...] += inner_rows(hid_ref[...], out_slope)
        pre_slope = (outer_cols(out_slope, wout_ref[...]) * slope_ref[...].astype(F32)).astype(BF)
        pre_all[pl.ds(pl.multiple_of(step * block, block), block), :] = pre_slope
        first_acc[...] += inner_rows(lat_ref[...], pre_slope)

    starts = [group[0].lo for group in edges]

    @pl.when(step == steps - 1)
    def _():
        pack[pl.ds(starts[0], d), :] = (first_acc[...] * factor).astype(BF)
        pack[pl.ds(starts[1], d), :] = (out_acc[...] * factor).astype(BF)
        for fold in groups["a"]:
            fold.begin(0)

    def scatter(kind, total):
        row = edge_index(tiles_ref, own, halo)[kind]
        at_block = pl.ds(pl.multiple_of(lax.rem(step, steps) * block, block), block)
        total[...] += product(one_hot(row, (rows, block), 0), pre_all[at_block, :])

    def weight_of(source):
        weight = None
        for part, lo in ((mesh_ref, 0), (halo_ref, own), (coarse_ref, own + halo)):
            term = inner_rows(part[...], source[pl.ds(lo, part.shape[0]), :].astype(BF))
            weight = term if weight is None else weight + term
        return (weight * factor).astype(BF)

    def back(lo, size):
        span = pl.ds(lo, size)
        return outer_cols(sent[span, :].astype(BF), win_ref[1]) + outer_cols(
            received[span, :].astype(BF), win_ref[2]
        )

    @pl.when(step // steps == 1)
    def _():
        scatter(3, received)

    @pl.when(step == 2 * steps - 1)
    def _():
        pack[pl.ds(starts[4], d), :] = weight_of(received)
        for fold in groups["b"]:
            fold.begin(0)

    @pl.when(step // steps == 2)
    def _():
        scatter(2, sent)

    slots = leaving.shape[1]

    def home_copy(k):
        return pltpu.make_async_remote_copy(
            src_ref=leaving.at[k],
            dst_ref=landed.at[k],
            send_sem=send.at[k],
            recv_sem=recv.at[k],
            device_id=block_at(place, sizes, moves[k]),
            device_id_type=MESH,
        )

    @pl.when(step == 3 * steps - 1)
    def _():
        pack[pl.ds(starts[2], coarse), :] = back(own + halo, coarse).astype(BF)
        at = 0
        for fold, span in zip(shares, spans):
            here_span = pl.ds(pl.multiple_of(starts[2] + span.start, 16), span.size)
            pack[here_span, :] = (
                pack[here_span, :].astype(F32) + direct_part[pl.ds(at, span.size), :]
            ).astype(BF)
            at += span.size
        rest = starts[3] - starts[2] - coarse
        which = lax.broadcasted_iota(jnp.int32, (rest, d), 0)
        pack[pl.ds(starts[2] + coarse, rest), :] = (
            jnp.where(which == 0, gain_acc[...], node_gain[...]) * factor
        ).astype(BF)
        for fold in groups["c"]:
            fold.begin(0)
        pack[pl.ds(starts[3], d), :] = weight_of(sent)
        for fold in groups["d"]:
            fold.begin(0)
        leave = back(own, halo).astype(BF)
        for k in range(len(moves)):
            leaving[k] = leave[k * slots : (k + 1) * slots]
        for k in range(len(moves)):
            home_copy(k).start()

    @pl.when(step // steps == 3)
    def _():
        at_block = pl.ds(pl.multiple_of((step - 3 * steps) * block, block), block)
        edges_grad[...] = (grad_ref[...].astype(F32) + outer_cols(pre_all[at_block, :], win_ref[0])).astype(BF)

    for part, names in table.items():

        @pl.when(step == part * 4 * steps // 16)
        def _():
            move(names)

    @pl.when(step == 4 * steps - 1)
    def _():
        direct = own_direct[...] + back(0, own)
        whole_coarse = pltpu.make_async_copy(new_coarse, coarse_out, coarse_sem)
        while wide + turns["n"] <= count:
            move("n")
        whole_coarse.start()
        while any(turn < 2 * count for turn in turns.values()):
            move("cdnab")
        for k in range(len(moves)):
            home_copy(k).wait()
        home = landed[...].reshape(halo, d)
        nodes_grad[...] = (direct + inner_rows(picks(lists_ref, own), home)).astype(BF)
        for name in groups:
            for fold in groups[name]:
                fold.delivery().wait()
                fold.drain()
        whole_coarse.wait()


def hand_out(
    starts,
    coarse,
    edge_sum,
    node_sum,
    new_coarse,
    nodes_grad,
    new_nodes,
    new_edges,
    edges_grad,
    edge_in,
    edge_out,
    coarse_grad,
    node_in,
    node_out,
    coarse_new,
    mesh_grad,
    mesh_new,
    edges_new,
    edges_back,
    edge_gain,
    node_gain,
    held,
    tail,
    come,
    leave,
    tail_sem,
):
    d = edge_sum.shape[1]
    last = pltpu.make_async_copy(edge_sum.at[pl.ds(starts[2] + coarse, tail.shape[0])], tail, tail_sem)
    last.start()
    jobs = hand_jobs(
        starts, coarse, edge_sum, node_sum, new_coarse, nodes_grad, new_nodes, new_edges, edges_grad, edge_in,
        edge_out, coarse_grad, node_in, node_out, coarse_new, mesh_grad, mesh_new, edges_new, edges_back,
    )
    moved, at = [], 0
    for number, (source, lo, target, target_lo, size) in enumerate(jobs):
        here_span = held.at[pl.ds(at, size)]
        at += size
        moved.append(
            (
                pltpu.make_async_copy(source.at[pl.ds(lo, size)], here_span, come.at[number]),
                pltpu.make_async_copy(here_span, target.at[pl.ds(target_lo, size)], leave.at[number]),
            )
        )
    for first, _ in moved:
        first.start()
    for first, second in moved:
        first.wait()
        second.start()
    last.wait()
    edge_gain[...] = tail[pl.ds(0, 1), :].astype(F32)
    node_gain[...] = tail[pl.ds(1, 1), :].astype(F32)
    for _, second in moved:
        second.wait()


def hand_jobs(
    starts, coarse, edge_sum, node_sum, new_coarse, nodes_grad, new_nodes, new_edges, edges_grad, edge_in,
    edge_out, coarse_grad, node_in, node_out, coarse_new, mesh_grad, mesh_new, edges_new, edges_back,
):
    d, own, edges = edge_sum.shape[1], new_nodes.shape[0], new_edges.shape[0]
    jobs = []
    for source, target in ((new_edges, edges_new), (edges_grad, edges_back)):
        jobs += [(source, lo, target, lo, d) for lo in range(0, edges, d)]
    jobs += [(node_sum, 0, node_in, 0, d), (node_sum, d, node_in, d, d), (node_sum, 2 * d, node_out, 0, d)]
    jobs += [(new_coarse, 0, coarse_new, 0, coarse), (new_nodes, 0, mesh_new, 0, own)]
    jobs += [(edge_sum, starts[0], edge_in, 0, d), (edge_sum, starts[3], edge_in, d, d)]
    jobs += [(edge_sum, starts[4], edge_in, 2 * d, d), (edge_sum, starts[1], edge_out, 0, d)]
    return jobs + [(edge_sum, starts[2], coarse_grad, 0, coarse), (nodes_grad, 0, mesh_grad, 0, own)]


def whole(shape):
    zero = (0,) * len(shape)
    return pl.BlockSpec(shape, lambda i: zero)


def by_rows(block, width):
    return pl.BlockSpec((block, width), lambda i: (i, 0))


def by_cols(block):
    return pl.BlockSpec((1, block), lambda i: (0, i))


def shape_of(shape, dtype):
    return jax.ShapeDtypeStruct(shape, dtype)


def cost(flops, moved):
    return pl.CostEstimate(flops=int(flops), bytes_accessed=int(moved), transcendentals=0)


PARAMS = dict(
    compiler_params=pltpu.CompilerParams(
        dimension_semantics=("arbitrary",), vmem_limit_bytes=60 * 1024 * 1024
    )
)


def talking(number, grid=False):
    return pltpu.CompilerParams(
        collective_id=number,
        has_side_effects=True,
        vmem_limit_bytes=60 * 1024 * 1024,
        dimension_semantics=("arbitrary",) if grid else None,
    )


def on_device(
    mesh_nodes,
    coarse_nodes,
    edge_latents,
    edge_tiles,
    send_lists,
    tiles_live,
    edge_in,
    edge_out,
    edge_gain,
    node_in,
    node_out,
    node_gain,
    grad_nodes,
    grad_coarse,
    grad_edges,
):
    sizes = tuple(lax.axis_size(axis) for axis in AXES)
    block_count = sizes[0] * sizes[1]
    bits = square_bits(sizes)
    count = len(bits)
    own, d = mesh_nodes.shape
    neigh, slots = send_lists.shape[1:]
    coarse = coarse_nodes.shape[0]
    halo = neigh * slots
    rows = own + halo + coarse
    tile_dev, _, tile_width = edge_tiles.shape
    edges = tile_dev * tile_width
    tiles = 4 if tile_dev % 4 == 0 else 1
    block = tiles * tile_width
    moves = cycle_moves(neigh, block_count)
    factor = float(edges * block_count) ** (-0.5)
    e_gain, n_gain = edge_gain.reshape(1, d), node_gain.reshape(1, d)
    vmem = pl.BlockSpec(memory_space=pltpu.VMEM)
    smem = pl.BlockSpec(memory_space=pltpu.SMEM)
    wide, col = by_rows(block, d), by_rows(block, 1)
    pairs = pl.BlockSpec((tiles, 2, tile_width), lambda i: (i, 0, 0))
    tables = [whole((own, d)), whole((halo, d)), whole((coarse, d))]
    weights = [whole((3, d, d)), whole((d, d)), whole((1, d))]
    swap = [pltpu.VMEM((neigh, slots, d), BF)] * 2 + [pltpu.SemaphoreType.DMA((neigh,))] * 2
    new_edges, hidden, slope, normed, inverse, agg_own, agg_coarse, incoming = pl.pallas_call(
        functools.partial(edge_forward, tile_width, sizes, moves),
        grid=(edges // block,),
        in_specs=[smem, wide, pairs, whole((1, neigh, slots)), tables[0], tables[2]] + weights,
        out_specs=[wide] * 4 + [col, tables[0], tables[2], tables[1]],
        out_shape=[shape_of((edges, d), BF)] * 4
        + [
            shape_of((edges, 1), F32),
            shape_of((own, d), BF),
            shape_of((coarse, d), BF),
            shape_of((halo, d), BF),
        ],
        scratch_shapes=[
            pltpu.VMEM((rows, d), BF),
            pltpu.VMEM((rows, d), BF),
            pltpu.VMEM((rows, d), F32),
            pltpu.VMEM((block, d), BF),
        ]
        + swap,
        cost_estimate=cost(2 * edges * d * (3 * rows + 2 * d), 12 * edges * d),
        compiler_params=talking(0, grid=True),
    )(
        tiles_live, edge_latents, edge_tiles, send_lists, mesh_nodes, coarse_nodes, edge_in, edge_out, e_gain
    )
    sum_rows = padded(coarse, count)
    grown = [agg_coarse, coarse_nodes, grad_coarse]
    if sum_rows > coarse:
        grown = [jnp.pad(array, ((0, sum_rows - coarse), (0, 0))) for array in grown]
    coarse_rows = split_rows(sum_rows, count, 3)
    share_rows = sum_rows // 2 ** (count - 2)
    all_rows = own + share_rows
    node_rows = padded(3 * d, count)
    parts = len(coarse_rows)
    new_nodes, new_part, own_slope, c_slope, own_direct, direct_part, node_pack, node_gain_part = pl.pallas_call(
        functools.partial(middle_step, bits, coarse_rows, factor),
        in_specs=[vmem] * 9,
        out_specs=[vmem] * 8,
        out_shape=[
            shape_of((own, d), BF),
            shape_of((share_rows, d), BF),
            shape_of((own, d), BF),
            shape_of((sum_rows, d), BF),
            shape_of((own, d), F32),
            shape_of((share_rows, d), F32),
            shape_of((node_rows, d), BF),
            shape_of((1, d), F32),
        ],
        scratch_shapes=[pltpu.VMEM((sum_rows, d), BF)]
        + [pltpu.VMEM((all_rows, d), BF)] * 5
        + [pltpu.SemaphoreType.DMA((parts, count))] * 2
        + fold_scratch(coarse_kinds(count), coarse_rows, d),
        compiler_params=talking(1),
    )(agg_own, grown[0], mesh_nodes, grown[1], grad_nodes, grown[2], node_in, node_out, n_gain)
    if sum_rows > coarse:
        c_slope = c_slope[:coarse]
    sections = [d, d, coarse + 2, d, d]
    edge_cuts = [split_rows(section, count, pieces) for section, pieces in zip(sections, (2, 2, 3, 4, 2))]
    node_cuts = split_rows(node_rows, count, 3)
    starts = [sum(sum(cuts) for cuts in edge_cuts[:i]) for i in range(len(sections))]
    edge_rows = sum(sum(cuts) for cuts in edge_cuts)
    steps = edges // block

    away = pl.BlockSpec(memory_space=pl.ANY)
    cuts = node_cuts + [size for section in edge_cuts for size in section]

    def once(width):
        return pl.BlockSpec((block, width), lambda i: (i - ((i // steps + 3) // 4) * (i - (steps - 1)), 0))

    again = pl.BlockSpec((block, d), lambda i: (lax.rem(i, steps), 0))
    again_pairs = pl.BlockSpec((tiles, 2, tile_width), lambda i: (lax.rem(i, steps), 0, 0))
    later = pl.BlockSpec((block, d), lambda i: ((i // (3 * steps)) * (i - 3 * steps), 0))
    edges_grad, edge_sum, node_sum, new_coarse, nodes_grad = pl.pallas_call(
        functools.partial(
            edge_backward, tile_width, factor, bits, sizes, moves, steps, node_cuts, edge_cuts, coarse_rows
        ),
        grid=(4 * steps,),
        in_specs=[smem, once(d), again] + [once(d)] * 3 + [once(1), again_pairs] + [vmem] * 14,
        out_specs=[later] + [away] * 3 + [vmem],
        out_shape=[
            shape_of((edges, d), BF),
            shape_of((edge_rows, d), BF),
            shape_of((node_rows, d), BF),
            shape_of((sum_rows, d), BF),
            shape_of((own, d), BF),
        ],
        scratch_shapes=[
            pltpu.VMEM((edge_rows, d), BF),
            pltpu.VMEM((node_rows, d), BF),
            pltpu.VMEM((sum_rows, d), BF),
            pltpu.SemaphoreType.DMA((len(cuts),)),
            pltpu.SemaphoreType.DMA,
            pltpu.VMEM((rows, d), BF),
            pltpu.VMEM((rows, d), F32),
            pltpu.VMEM((rows, d), F32),
            pltpu.VMEM((d, d), F32),
            pltpu.VMEM((d, d), F32),
            pltpu.VMEM((1, d), F32),
            pltpu.VMEM((edges, d), BF),
            pltpu.VMEM((edge_rows, d), BF),
        ]
        + swap
        + [pltpu.SemaphoreType.DMA((parts, count))] * 2
        + fold_scratch(sum_kinds(count), cuts, d),
        cost_estimate=cost(2 * edges * d * (3 * rows + 4 * d), 14 * edges * d),
        compiler_params=talking(2, grid=True),
    )(
        tiles_live, edge_latents, grad_edges, hidden, slope, normed, inverse, edge_tiles, mesh_nodes, incoming,
        coarse_nodes, own_slope, c_slope, own_direct, direct_part, new_part, node_pack, node_gain_part, send_lists,
        edge_in, edge_out, e_gain,
    )
    sources = [edge_sum, node_sum, new_coarse, nodes_grad, new_nodes, new_edges, edges_grad]
    results = [
        shape_of((3 * d, d), BF),
        shape_of((d, d), BF),
        shape_of((coarse, d), BF),
        shape_of((2 * d, d), BF),
        shape_of((d, d), BF),
        shape_of((coarse, d), BF),
        shape_of((own, d), BF),
        shape_of((own, d), BF),
        shape_of((edges, d), BF),
        shape_of((edges, d), BF),
    ]
    jobs = hand_jobs(starts, coarse, *sources, *results)
    (
        g_in,
        g_out,
        coarse_grad,
        n_in,
        n_out,
        coarse_new,
        mesh_grad,
        mesh_new,
        new_edges,
        edges_grad,
        edge_gain_grad,
        node_gain_grad,
    ) = pl.pallas_call(
        functools.partial(hand_out, starts, coarse),
        in_specs=[away] * len(sources),
        out_specs=[away] * len(results) + [vmem] * 2,
        out_shape=results + [shape_of((1, d), F32)] * 2,
        scratch_shapes=[
            pltpu.VMEM((sum(job[-1] for job in jobs), d), BF),
            pltpu.VMEM((16, d), BF),
            pltpu.SemaphoreType.DMA((len(jobs),)),
            pltpu.SemaphoreType.DMA((len(jobs),)),
            pltpu.SemaphoreType.DMA,
        ],
        compiler_params=pltpu.CompilerParams(vmem_limit_bytes=60 * 1024 * 1024),
    )(*sources)
    return (
        mesh_new,
        coarse_new,
        new_edges,
        mesh_grad,
        coarse_grad,
        edges_grad,
        g_in.reshape(3, d, d),
        g_out,
        edge_gain_grad[0],
        n_in.reshape(2, d, d),
        n_out,
        node_gain_grad[0],
    )


def solution(mesh):
    rows2 = P(AXES, None)
    rows3 = P(AXES, None, None)
    in_specs = (
        rows2, P(), rows2, rows3, rows3, P(AXES), P(), P(), P(), P(), P(), P(), rows2, P(), rows2,
    )
    out_specs = (rows2, P(), rows2, rows2, P(), rows2, P(), P(), P(), P(), P(), P())
    return jax.shard_map(
        on_device, mesh=mesh, in_specs=in_specs, out_specs=out_specs, check_vma=False
    )
```
